128 devices in a mesh: zero: 8 (over x, core), width: 16 (over z, y).
Axes of the slice: x: 4, y: 4, z: 4, core: 2. Of those that a mesh axis runs over, the one named last changes fastest.
Arguments:
- weight_query: float32 [8192, 8192], P('zero', 'width'), may hold values from -0.09375 to 0.09375
- smooth_query: float32 [8192, 8192], P('zero', 'width'), may hold values from -0.0625 to 0.0625
- weight_key: float32 [8192, 512], P('zero', 'width'), may hold values from -0.09375 to 0.09375
- smooth_key: float32 [8192, 512], P('zero', 'width'), may hold values from -0.0625 to 0.0625
- weight_value: float32 [8192, 512], P('zero', 'width'), may hold values from -0.09375 to 0.09375
- smooth_value: float32 [8192, 512], P('zero', 'width'), may hold values from -0.0625 to 0.0625
- norm_train: float32 [8192], P(('zero', 'width')), may hold values from 0.25 to 1.75
- norm_step: float32 [8192], P(('zero', 'width')), may hold values from -0.3 to 0.3
Outputs:
- final_query: bfloat16 [8192, 8192], P(None, 'width')
- final_key: bfloat16 [8192, 512], P(None, 'width')
- final_value: bfloat16 [8192, 512], P(None, 'width')
- factor_query: float32 [8192], P('width')
- factor_key: float32 [512], P('width')
- factor_value: float32 [512], P('width')
- serve_norm: bfloat16 [8192], replicated
- result_query: float32 [8192, 8192], P('zero', 'width')
- result_key: float32 [8192, 512], P('zero', 'width')
- result_value: float32 [8192, 512], P('zero', 'width')
The draws below stay inside these ranges and needn't reach their ends.
All inputs are finite; a program needn't handle non-finite values. Where the reference program divides by a largest or mean magnitude, that divisor is 1e-20 or more.
Results may differ from the reference program's by a relative error of at most 0.001.
Values may be sent and summed in bfloat16 or wider, within the bound.
A program may use at most 128 MiB of HBM per device.

```python
import jax
import jax.numpy as jnp

D_MODEL = 8192
Q_DIM = 8192
KV_DIM = 512


def with_spikes(array, stream_key, source, target, shards_of, factor):
    owner, partner = [(jnp.arange(array.shape[position]) // (array.shape[position] // shards_of)).reshape([-1 if axis == position else 1 for axis in range(array.ndim)]) for position in (source, target)]
    chosen = jax.random.permutation(stream_key, shards_of)[partner]
    strong = (owner == chosen) | (owner == (partner + shards_of // 2) % shards_of)
    return jnp.where(strong, factor * array, array)


def block_scale(own_key, dims, shards, least, high):
    level, own = 1.0, jax.random.fold_in(own_key, 6)
    for axis_at, shards_of in shards:
        draws = jnp.exp(jax.random.uniform(jax.random.fold_in(own, axis_at), (shards_of,), jnp.float32, least / len(shards), high / len(shards)))
        level = level * jnp.repeat(draws, dims[axis_at] // shards_of).reshape([-1 if axis == axis_at else 1 for axis in range(len(dims))])
    return level


def normal_values(stream_key, extent, spread, limit, pieces=(), dtype=jnp.bfloat16):
    values = jax.random.normal(stream_key, extent, jnp.float32) * spread
    if len(pieces) > 0:
        values = block_scale(stream_key, extent, pieces, -0.22, 0.18) * values
    return jnp.clip(values, min=-limit, max=limit).astype(dtype)


def gaussian_with(rng, shape, width, most, cuts, heavy, kind=jnp.bfloat16):
    drawn = width * jax.random.normal(rng, shape, jnp.float32)
    if cuts:
        drawn = drawn * block_scale(rng, shape, cuts, -0.22, 0.18)
    return jnp.clip(with_spikes(drawn, jax.random.fold_in(rng, 3), *heavy), -most, most).astype(kind)


def setup_inputs(seed: int = 0) -> dict:
    key_list = jax.random.split(jax.random.key(seed), 9)
    return {
        "weight_query": gaussian_with(key_list[0], (D_MODEL, Q_DIM), D_MODEL ** -0.5, 0.09375, ((0, 8), (1, 16)), (0, 1, 16, 2.0), jnp.float32),
        "smooth_query": normal_values(key_list[1], (D_MODEL, Q_DIM), D_MODEL ** -0.5, 0.0625, ((0, 8), (1, 16)), jnp.float32),
        "weight_key": gaussian_with(key_list[2], (D_MODEL, KV_DIM), D_MODEL ** -0.5, 0.09375, ((0, 8), (1, 16)), (0, 1, 16, 2.0), jnp.float32),
        "smooth_key": normal_values(key_list[3], (D_MODEL, KV_DIM), D_MODEL ** -0.5, 0.0625, ((0, 8), (1, 16)), jnp.float32),
        "weight_value": gaussian_with(key_list[4], (D_MODEL, KV_DIM), D_MODEL ** -0.5, 0.09375, ((0, 8), (1, 16)), (0, 1, 16, 2.0), jnp.float32),
        "smooth_value": normal_values(key_list[5], (D_MODEL, KV_DIM), D_MODEL ** -0.5, 0.0625, ((0, 8), (1, 16)), jnp.float32),
        "norm_train": jnp.clip(1.0 + 0.15 * jax.random.normal(key_list[6], (D_MODEL,), jnp.float32), 0.25, 1.75),
        "norm_step": jnp.clip(jax.random.uniform(key_list[7], (D_MODEL,), jnp.float32, -0.3, 0.3) * block_scale(key_list[7], (D_MODEL,), ((0, 128),), -0.4, 0.0), -0.3, 0.3),
    }


keep_rate = 0.7


def reference(weight_query, smooth_query, weight_key, smooth_key, weight_value, smooth_value, norm_train, norm_step):
    result_query = keep_rate * smooth_query + (1.0 - keep_rate) * weight_query
    result_key = keep_rate * smooth_key + (1.0 - keep_rate) * weight_key
    result_value = keep_rate * smooth_value + (1.0 - keep_rate) * weight_value
    factor_query = jnp.sum(jnp.abs(result_query), axis=0) / D_MODEL
    final_query = (result_query / factor_query).astype(jnp.bfloat16)
    factor_key = jnp.sum(jnp.abs(result_key), axis=0) / D_MODEL
    final_key = (result_key / factor_key).astype(jnp.bfloat16)
    factor_value = jnp.sum(jnp.abs(result_value), axis=0) / D_MODEL
    final_value = (result_value / factor_value).astype(jnp.bfloat16)
    serve_norm = (norm_train + norm_step).astype(jnp.bfloat16)
    return final_query, final_key, final_value, factor_query, factor_key, factor_value, serve_norm, result_query, result_key, result_value
```

```python
import jax
import jax.numpy as jnp
from jax import lax
from jax.experimental import pallas as pl
from jax.experimental.pallas import tpu as pltpu
from jax.sharding import Mesh
from jax.sharding import PartitionSpec as P

D_MODEL = 8192
ZERO = ("zero_0", "zero_1")
ZERO_WIDTH = ("zero_0", "zero_1", "width_0", "width_1")
WIDTH = ("width_0", "width_1")
MESH = pl.DeviceIdType.MESH

keep_rate = 0.7

ROWS = 1024
COLS = 512
HALF = ROWS // 2
KV = 64
LANES = 128
TILES = COLS // LANES
STEP = 128
KV_ROW, NORM_ROW = TILES, TILES + 1
SUM_ROWS = TILES + 2

UNITS = tuple((tile, half) for tile in range(TILES + 1) for half in range(2))


def mix(smooth, weight):
    return keep_rate * smooth + (1.0 - keep_rate) * weight


def gather_kernel(
    wq, sq, wk, sk, wv, sv, norm_a, norm_b,
    out_q, out_kv, res_q, res_kv, fac_q, fac_k, fac_v, norm_out,
    wq_v, sq_v, wkv_v, skv_v, inv, sums, norm_y, norm_z, norm_all,
    in_sem, sum_send, sum_recv, own_send, fwd_send, rel_send,
    side_recv, far_recv, rel_recv, norm_send, norm_recv,
):
    x, c = lax.axis_index("zero_0"), lax.axis_index("zero_1")
    z, y = lax.axis_index("width_0"), lax.axis_index("width_1")
    me = x * 2 + c
    right, left = lax.rem(x + 1, 4), lax.rem(x + 3, 4)
    sides = ((left, right), (right, left))

    loads = []

    def load(src, dst):
        copy = pltpu.make_async_copy(src, dst, in_sem.at[len(loads)])
        copy.start()
        loads.append(copy)

    for t in range(TILES):
        cols = pl.ds(t * LANES, LANES)
        load(wq.at[:, cols], wq_v.at[:, cols])
        load(sq.at[:, cols], sq_v.at[:, cols])
    load(wk, wkv_v.at[pl.ds(0, 32), :])
    load(sk, skv_v.at[pl.ds(0, 32), :])
    load(wv, wkv_v.at[pl.ds(32, 32), :])
    load(sv, skv_v.at[pl.ds(32, 32), :])

    def group_peer(d):
        other = lax.rem(me + d, 8)
        return {"zero_0": other // 2, "zero_1": lax.rem(other, 2)}

    barrier = pltpu.get_barrier_semaphore()
    for d in (4, 5, 3, 2, 6, 7, 1):
        pl.semaphore_signal(barrier, inc=1, device_id=group_peer(d), device_id_type=MESH)
    for d in (2, 1, 3):
        pl.semaphore_signal(barrier, inc=1, device_id={"width_1": lax.rem(y + d, 4)}, device_id_type=MESH)
        pl.semaphore_signal(barrier, inc=1, device_id={"width_0": lax.rem(z + d, 4)}, device_id_type=MESH)

    def sum_tile(t):
        loads[2 * t].wait()
        loads[2 * t + 1].wait()
        cols = pl.ds(t * LANES, LANES)

        def body(i, acc):
            rows = pl.ds(pl.multiple_of(i * STEP, STEP), STEP)
            r = mix(sq_v[rows, cols], wq_v[rows, cols])
            res_q[rows, cols] = r
            return acc + jnp.sum(jnp.abs(r).reshape(STEP // 8, 8, LANES), axis=0)

        acc = lax.fori_loop(0, ROWS // STEP, body, jnp.zeros((8, LANES), jnp.float32))
        sums[me, t] = jnp.sum(acc, axis=0, keepdims=True)

    def send_sums(first, count, which):
        for d in (4, 5, 3, 2, 6, 7, 1):
            pltpu.make_async_remote_copy(
                src_ref=sums.at[me, pl.ds(first, count)],
                dst_ref=sums.at[me, pl.ds(first, count)],
                send_sem=sum_send.at[which, d],
                recv_sem=sum_recv.at[which, d],
                device_id=group_peer(d),
                device_id_type=MESH,
            ).start()

    def sums_copy(first, count, which, d):
        other = lax.rem(me + 8 - d, 8)
        return pltpu.make_async_remote_copy(
            src_ref=sums.at[other, pl.ds(first, count)],
            dst_ref=sums.at[other, pl.ds(first, count)],
            send_sem=sum_send.at[which, d],
            recv_sem=sum_recv.at[which, d],
            device_id=group_peer(d),
            device_id_type=MESH,
        )

    lane_of = lax.broadcasted_iota(jnp.int32, (KV, LANES), 1)
    diagonal = lane_of == lax.broadcasted_iota(jnp.int32, (KV, LANES), 0)

    sum_tile(0)
    pl.semaphore_wait(barrier, 13)
    send_sums(0, 1, 0)
    for t in range(1, TILES):
        sum_tile(t)
    for copy in loads[2 * TILES :]:
        copy.wait()
    acc = jnp.zeros((KV, LANES), jnp.float32)
    for j in range(ROWS // LANES):
        cols = pl.ds(j * LANES, LANES)
        r = mix(skv_v[:, cols], wkv_v[:, cols])
        res_kv[:, cols] = r
        acc = acc + jnp.abs(r)
    row_sums = jnp.sum(acc, axis=1, keepdims=True)
    sums[me, KV_ROW] = jnp.sum(jnp.where(diagonal, row_sums, 0.0), axis=0, keepdims=True)
    own_norm = norm_a[...] + norm_b[...]
    sums[me, NORM_ROW] = jnp.concatenate([own_norm, own_norm], axis=1)
    send_sums(1, SUM_ROWS - 1, 1)

    def place(origin, k):
        tile, half = UNITS[k]
        if tile < TILES:
            rows = pl.ds(pl.multiple_of(origin * ROWS + half * HALF, HALF), HALF)
            return out_q.at[rows, pl.ds(tile * LANES, LANES)]
        return out_kv.at[:, pl.ds(pl.multiple_of(origin * ROWS + half * HALF, HALF), HALF)]

    def unit_copy(origin, k, send_sem, recv_sem, device):
        ref = place(origin, k)
        return pltpu.make_async_remote_copy(
            src_ref=ref, dst_ref=ref, send_sem=send_sem, recv_sem=recv_sem, device_id=device, device_id_type=MESH
        )

    partner = {"zero_1": 1 - c}
    to_right, to_left = {"zero_0": right}, {"zero_0": left}
    sends = []

    def send(copy):
        copy.start()
        sends.append(copy)

    def send_own(k):
        ways = [(0, to_right), (1, to_left)]
        for side, device in ways if UNITS[k][1] == 0 else ways[::-1]:
            send(unit_copy(me, k, own_send.at[side, k], side_recv.at[side, k], device))
        send(unit_copy(me, k, own_send.at[2, k], rel_recv.at[0, k], partner))

    def narrow_tile(t):
        total = sums[0, t]
        for other in range(1, 8):
            total = total + sums[other, t]
        factor = total * (1.0 / D_MODEL)
        if t < TILES:
            fac_q[:, pl.ds(t * LANES, LANES)] = factor
            scale = 1.0 / factor
        else:
            fac_k[...] = factor[:, 0:32]
            fac_v[...] = pltpu.roll(factor, LANES - 32, 1)[:, 0:32]
            spread = jnp.sum(jnp.where(diagonal, jnp.broadcast_to(factor, (KV, LANES)), 0.0), axis=1, keepdims=True)
            scale = 1.0 / jnp.broadcast_to(spread, (KV, LANES))
        for half in range(2):
            if t < TILES:
                cols = pl.ds(t * LANES, LANES)

                def body(i, carry):
                    at = half * HALF + i * STEP
                    rows = pl.ds(pl.multiple_of(at, STEP), STEP)
                    there = pl.ds(pl.multiple_of(me * ROWS + at, STEP), STEP)
                    out_q[there, cols] = (res_q[rows, cols] * scale).astype(jnp.bfloat16)
                    return carry

                lax.fori_loop(0, HALF // STEP, body, 0)
            else:
                for j in range(HALF // LANES):
                    at = half * HALF + j * LANES
                    there = pl.ds(pl.multiple_of(me * ROWS + at, LANES), LANES)
                    out_kv[:, there] = (res_kv[:, pl.ds(at, LANES)] * scale).astype(jnp.bfloat16)
            send_own(2 * t + half)

    for d in range(1, 8):
        sums_copy(0, 1, 0, d).wait_recv()
    narrow_tile(0)
    for d in range(1, 8):
        sums_copy(1, SUM_ROWS - 1, 1, d).wait_recv()
    for t in range(1, TILES + 1):
        narrow_tile(t)

    def norm_copy(buf, at, stage, d, axis, here):
        return pltpu.make_async_remote_copy(
            src_ref=buf.at[at],
            dst_ref=buf.at[at],
            send_sem=norm_send.at[stage, d],
            recv_sem=norm_recv.at[stage, d],
            device_id={axis: lax.rem(here + d, 4)},
            device_id_type=MESH,
        )

    for other in range(8):
        norm_y[y, pl.ds(other, 1), :] = sums[other, NORM_ROW]
    for d in (2, 1, 3):
        norm_copy(norm_y, y, 0, d, "width_1", y).start()

    def norm_along_z():
        for d in (1, 3, 2):
            norm_copy(norm_y, lax.rem(y + 4 - d, 4), 0, d, "width_1", y).wait_recv()
        low = lax.broadcasted_iota(jnp.int32, (8, LANES), 1) < 64
        norm_z[z, 0] = jnp.where(low, norm_y[0], norm_y[1])
        norm_z[z, 1] = jnp.where(low, norm_y[2], norm_y[3])
        for d in (2, 1, 3):
            norm_copy(norm_z, z, 1, d, "width_0", z).start()

    def norm_end():
        for d in (1, 3, 2):
            norm_copy(norm_z, lax.rem(z + 4 - d, 4), 1, d, "width_0", z).wait_recv()
        for zz in range(4):
            for pair in range(2):
                for other in range(8):
                    norm_all[pl.ds(other * 8 + zz * 2 + pair, 1), :] = norm_z[zz, pair, pl.ds(other, 1), :]
        norm_out[...] = norm_all[...].astype(jnp.bfloat16)
        for d in range(1, 4):
            norm_copy(norm_y, y, 0, d, "width_1", y).wait_send()
            norm_copy(norm_z, z, 1, d, "width_0", z).wait_send()

    far = lax.rem(x + 2, 4)
    for k in range(len(UNITS)):
        for side in range(2):
            origin = (left if side == 0 else right) * 2 + c
            unit_copy(origin, k, own_send.at[side, k], side_recv.at[side, k], to_right).wait_recv()
            if UNITS[k][1] == side:
                send(unit_copy(origin, k, fwd_send.at[k], far_recv.at[k], to_right if side == 0 else to_left))
            send(unit_copy(origin, k, rel_send.at[side, k], rel_recv.at[1 + side, k], partner))
        if k == 2:
            norm_along_z()
        if k == 4:
            norm_end()
    for k in range(len(UNITS)):
        unit_copy(far * 2 + c, k, fwd_send.at[k], far_recv.at[k], to_right).wait_recv()
        send(unit_copy(far * 2 + c, k, rel_send.at[2, k], rel_recv.at[3, k], partner))

    for d in range(1, 8):
        sums_copy(0, 1, 0, d).wait_send()
        sums_copy(1, SUM_ROWS - 1, 1, d).wait_send()
    for copy in sends:
        copy.wait_send()
    for which, origin in enumerate((x, left, right, far)):
        for k in range(len(UNITS)):
            unit_copy(origin * 2 + 1 - c, k, own_send.at[2, k], rel_recv.at[which, k], partner).wait_recv()


def write_kernel(
    out_q, out_kv, res_q, res_kv, fac_q, fac_k, fac_v, norm,
    final_q, final_k, final_v, factor_q, factor_k, factor_v, serve_norm, result_q, result_k, result_v, sem,
):
    copies = []

    def write(src, dst):
        copy = pltpu.make_async_copy(src, dst, sem.at[len(copies)])
        copy.start()
        copies.append(copy)

    for part in range(8):
        rows = pl.ds(part * ROWS, ROWS)
        write(out_q.at[rows, :], final_q.at[rows, :])
    write(res_q, result_q)
    write(out_kv.at[pl.ds(0, 32), :], final_k)
    write(out_kv.at[pl.ds(32, 32), :], final_v)
    write(res_kv.at[pl.ds(0, 32), :], result_k)
    write(res_kv.at[pl.ds(32, 32), :], result_v)
    write(fac_q, factor_q)
    write(fac_k, factor_k)
    write(fac_v, factor_v)
    write(norm, serve_norm)
    for copy in copies:
        copy.wait()


def on_device(weight_query, smooth_query, weight_key, smooth_key, weight_value, smooth_value, norm_train, norm_step):
    f32, bf16 = jnp.float32, jnp.bfloat16
    any_spec, vmem_spec = pl.BlockSpec(memory_space=pl.ANY), pl.BlockSpec(memory_space=pltpu.VMEM)
    held = (
        ((D_MODEL, COLS), bf16),
        ((KV, D_MODEL), bf16),
        ((ROWS, COLS), f32),
        ((KV, ROWS), f32),
        ((1, COLS), f32),
        ((1, 32), f32),
        ((1, 32), f32),
        ((64, LANES), bf16),
    )
    units = len(UNITS)
    dma = pltpu.SemaphoreType.DMA
    gathered = pl.pallas_call(
        gather_kernel,
        out_shape=tuple(pltpu.VMEM(shape, dtype) for shape, dtype in held),
        in_specs=[any_spec] * 6 + [vmem_spec] * 2,
        out_specs=tuple(vmem_spec for _ in held),
        scratch_shapes=[
            pltpu.VMEM((ROWS, COLS), f32),
            pltpu.VMEM((ROWS, COLS), f32),
            pltpu.VMEM((KV, ROWS), f32),
            pltpu.VMEM((KV, ROWS), f32),
            pltpu.VMEM((1, COLS), f32),
            pltpu.VMEM((8, SUM_ROWS, 1, LANES), f32),
            pltpu.VMEM((4, 8, LANES), f32),
            pltpu.VMEM((4, 2, 8, LANES), f32),
            pltpu.VMEM((64, LANES), f32),
            dma((2 * TILES + 4,)),
            dma((2, 8)),
            dma((2, 8)),
            dma((3, units)),
            dma((units,)),
            dma((3, units)),
            dma((2, units)),
            dma((units,)),
            dma((4, units)),
            dma((2, 4)),
            dma((2, 4)),
        ],
        compiler_params=pltpu.CompilerParams(
            collective_id=0, has_side_effects=True, vmem_limit_bytes=16 * 1024 * 1024
        ),
        name="gather",
    )(
        weight_query, smooth_query, weight_key.T, smooth_key.T, weight_value.T, smooth_value.T,
        norm_train.reshape(1, 64), norm_step.reshape(1, 64),
    )
    outs = (
        ((D_MODEL, COLS), bf16),
        ((32, D_MODEL), bf16),
        ((32, D_MODEL), bf16),
        ((1, COLS), f32),
        ((1, 32), f32),
        ((1, 32), f32),
        ((64, LANES), bf16),
        ((ROWS, COLS), f32),
        ((32, ROWS), f32),
        ((32, ROWS), f32),
    )
    fq, fk, fv, cq, ck, cv, norm, rq, rk, rv = pl.pallas_call(
        write_kernel,
        out_shape=tuple(jax.ShapeDtypeStruct(shape, dtype) for shape, dtype in outs),
        in_specs=[vmem_spec] * len(held),
        out_specs=tuple(any_spec for _ in outs),
        scratch_shapes=[dma((17,))],
        compiler_params=pltpu.CompilerParams(vmem_limit_bytes=4 * 1024 * 1024),
        name="write",
    )(*gathered)
    return (
        fq, fk.T, fv.T, cq.reshape(COLS), ck.reshape(32), cv.reshape(32), norm.reshape(D_MODEL), rq, rk.T, rv.T
    )


def solution(mesh):
    split = Mesh(mesh.devices.reshape(4, 2, 4, 4), ("zero_0", "zero_1", "width_0", "width_1"))
    in_specs = (
        P(ZERO, WIDTH),
        P(ZERO, WIDTH),
        P(ZERO, WIDTH),
        P(ZERO, WIDTH),
        P(ZERO, WIDTH),
        P(ZERO, WIDTH),
        P(ZERO_WIDTH),
        P(ZERO_WIDTH),
    )
    out_specs = (
        P(None, WIDTH),
        P(None, WIDTH),
        P(None, WIDTH),
        P(WIDTH),
        P(WIDTH),
        P(WIDTH),
        P(),
        P(ZERO, WIDTH),
        P(ZERO, WIDTH),
        P(ZERO, WIDTH),
    )
    return jax.shard_map(
        on_device, mesh=split, in_specs=in_specs, out_specs=out_specs, check_vma=False
    )
```

```python
import jax
import jax.numpy as jnp
from jax import lax
from jax.experimental import pallas as pl
from jax.experimental.pallas import tpu as pltpu
from jax.sharding import Mesh
from jax.sharding import PartitionSpec as P

D_MODEL = 8192
ZERO = ("zero_0", "zero_1")
ZERO_WIDTH = ("zero_0", "zero_1", "width_0", "width_1")
WIDTH = ("width_0", "width_1")
MESH = pl.DeviceIdType.MESH

keep_rate = 0.7

ROWS = 1024
COLS = 512
HALF = ROWS // 2
KV = 64
LANES = 128
TILES = COLS // LANES
STEP = 128
KV_ROW, NORM_ROW = TILES, TILES + 1
SUM_ROWS = TILES + 2

UNITS = tuple((tile, half) for tile in range(TILES + 1) for half in range(2))


def mix(smooth, weight):
    return keep_rate * smooth + (1.0 - keep_rate) * weight


def gather_kernel(
    wq, sq, wk, sk, wv, sv, norm_a, norm_b,
    out_q, out_kv, res_q, res_kv, fac_q, fac_k, fac_v, norm_out,
    wq_v, sq_v, wkv_v, skv_v, norm_v, sums, norm_y, norm_z, norm_all,
    in_sem, sum_send, sum_recv, own_send, fwd_send, rel_send,
    side_recv, far_recv, rel_recv, norm_send, norm_recv,
):
    x, c = lax.axis_index("zero_0"), lax.axis_index("zero_1")
    z, y = lax.axis_index("width_0"), lax.axis_index("width_1")
    me = x * 2 + c
    right, left = lax.rem(x + 1, 4), lax.rem(x + 3, 4)
    sides = ((left, right), (right, left))

    loads = []

    def load(src, dst):
        copy = pltpu.make_async_copy(src, dst, in_sem.at[len(loads)])
        copy.start()
        loads.append(copy)

    for t in range(TILES):
        cols = pl.ds(t * LANES, LANES)
        load(wq.at[:, cols], wq_v.at[:, cols])
        load(sq.at[:, cols], sq_v.at[:, cols])
    load(wk, wkv_v.at[pl.ds(0, 32), :])
    load(sk, skv_v.at[pl.ds(0, 32), :])
    load(wv, wkv_v.at[pl.ds(32, 32), :])
    load(sv, skv_v.at[pl.ds(32, 32), :])
    load(norm_a, norm_v.at[0])
    load(norm_b, norm_v.at[1])

    def group_peer(d):
        other = lax.rem(me + d, 8)
        return {"zero_0": other // 2, "zero_1": lax.rem(other, 2)}

    barrier = pltpu.get_barrier_semaphore()
    for d in (4, 5, 3, 2, 6, 7, 1):
        pl.semaphore_signal(barrier, inc=1, device_id=group_peer(d), device_id_type=MESH)
    for d in (2, 1, 3):
        pl.semaphore_signal(barrier, inc=1, device_id={"width_1": lax.rem(y + d, 4)}, device_id_type=MESH)
        pl.semaphore_signal(barrier, inc=1, device_id={"width_0": lax.rem(z + d, 4)}, device_id_type=MESH)

    def sum_tile(t):
        loads[2 * t].wait()
        loads[2 * t + 1].wait()
        cols = pl.ds(t * LANES, LANES)

        def body(i, acc):
            rows = pl.ds(pl.multiple_of(i * STEP, STEP), STEP)
            r = mix(sq_v[rows, cols], wq_v[rows, cols])
            res_q[rows, cols] = r
            return acc + jnp.sum(jnp.abs(r).reshape(STEP // 8, 8, LANES), axis=0)

        acc = lax.fori_loop(0, ROWS // STEP, body, jnp.zeros((8, LANES), jnp.float32))
        sums[me, t] = jnp.sum(acc, axis=0, keepdims=True)

    def send_sums(first, count, which):
        for d in (4, 5, 3, 2, 6, 7, 1):
            pltpu.make_async_remote_copy(
                src_ref=sums.at[me, pl.ds(first, count)],
                dst_ref=sums.at[me, pl.ds(first, count)],
                send_sem=sum_send.at[which, d],
                recv_sem=sum_recv.at[which, d],
                device_id=group_peer(d),
                device_id_type=MESH,
            ).start()

    def sums_copy(first, count, which, d):
        other = lax.rem(me + 8 - d, 8)
        return pltpu.make_async_remote_copy(
            src_ref=sums.at[other, pl.ds(first, count)],
            dst_ref=sums.at[other, pl.ds(first, count)],
            send_sem=sum_send.at[which, d],
            recv_sem=sum_recv.at[which, d],
            device_id=group_peer(d),
            device_id_type=MESH,
        )

    lane_of = lax.broadcasted_iota(jnp.int32, (KV, LANES), 1)
    diagonal = lane_of == lax.broadcasted_iota(jnp.int32, (KV, LANES), 0)

    sum_tile(0)
    pl.semaphore_wait(barrier, 13)
    send_sums(0, 1, 0)
    for t in range(1, TILES):
        sum_tile(t)
    for copy in loads[2 * TILES :]:
        copy.wait()
    acc = jnp.zeros((KV, LANES), jnp.float32)
    for j in range(ROWS // LANES):
        cols = pl.ds(j * LANES, LANES)
        r = mix(skv_v[:, cols], wkv_v[:, cols])
        res_kv[:, cols] = r
        acc = acc + jnp.abs(r)
    row_sums = jnp.sum(acc, axis=1, keepdims=True)
    sums[me, KV_ROW] = jnp.sum(jnp.where(diagonal, row_sums, 0.0), axis=0, keepdims=True)
    own_norm = norm_v[0] + norm_v[1]
    sums[me, NORM_ROW] = jnp.concatenate([own_norm, own_norm], axis=1)
    send_sums(1, SUM_ROWS - 1, 1)

    def place(origin, k):
        tile, half = UNITS[k]
        if tile < TILES:
            rows = pl.ds(pl.multiple_of(origin * ROWS + half * HALF, HALF), HALF)
            return out_q.at[rows, pl.ds(tile * LANES, LANES)]
        return out_kv.at[:, pl.ds(pl.multiple_of(origin * ROWS + half * HALF, HALF), HALF)]

    def unit_copy(origin, k, send_sem, recv_sem, device):
        ref = place(origin, k)
        return pltpu.make_async_remote_copy(
            src_ref=ref, dst_ref=ref, send_sem=send_sem, recv_sem=recv_sem, device_id=device, device_id_type=MESH
        )

    partner = {"zero_1": 1 - c}
    to_right, to_left = {"zero_0": right}, {"zero_0": left}
    sends = []

    def send(copy):
        copy.start()
        sends.append(copy)

    def send_own(k):
        ways = [(0, to_right), (1, to_left)]
        for side, device in ways if UNITS[k][1] == 0 else ways[::-1]:
            send(unit_copy(me, k, own_send.at[side, k], side_recv.at[side, k], device))
        send(unit_copy(me, k, own_send.at[2, k], rel_recv.at[0, k], partner))

    def narrow_tile(t):
        total = sums[0, t]
        for other in range(1, 8):
            total = total + sums[other, t]
        factor = total * (1.0 / D_MODEL)
        if t < TILES:
            fac_q[:, pl.ds(t * LANES, LANES)] = factor
            scale = 1.0 / factor
        else:
            fac_k[...] = factor[:, 0:32]
            fac_v[...] = pltpu.roll(factor, LANES - 32, 1)[:, 0:32]
            spread = jnp.sum(jnp.where(diagonal, jnp.broadcast_to(factor, (KV, LANES)), 0.0), axis=1, keepdims=True)
            scale = 1.0 / jnp.broadcast_to(spread, (KV, LANES))
        for half in range(2):
            if t < TILES:
                cols = pl.ds(t * LANES, LANES)

                def body(i, carry):
                    at = half * HALF + i * STEP
                    rows = pl.ds(pl.multiple_of(at, STEP), STEP)
                    there = pl.ds(pl.multiple_of(me * ROWS + at, STEP), STEP)
                    out_q[there, cols] = (res_q[rows, cols] * scale).astype(jnp.bfloat16)
                    return carry

                lax.fori_loop(0, HALF // STEP, body, 0)
            else:
                for j in range(HALF // LANES):
                    at = half * HALF + j * LANES
                    there = pl.ds(pl.multiple_of(me * ROWS + at, LANES), LANES)
                    out_kv[:, there] = (res_kv[:, pl.ds(at, LANES)] * scale).astype(jnp.bfloat16)
            send_own(2 * t + half)

    for d in range(1, 8):
        sums_copy(0, 1, 0, d).wait_recv()
    narrow_tile(0)
    for d in range(1, 8):
        sums_copy(1, SUM_ROWS - 1, 1, d).wait_recv()
    for t in range(1, TILES + 1):
        narrow_tile(t)

    def norm_copy(buf, at, stage, d, axis, here):
        return pltpu.make_async_remote_copy(
            src_ref=buf.at[at],
            dst_ref=buf.at[at],
            send_sem=norm_send.at[stage, d],
            recv_sem=norm_recv.at[stage, d],
            device_id={axis: lax.rem(here + d, 4)},
            device_id_type=MESH,
        )

    for other in range(8):
        norm_y[y, pl.ds(other, 1), :] = sums[other, NORM_ROW]
    for d in (2, 1, 3):
        norm_copy(norm_y, y, 0, d, "width_1", y).start()

    def norm_along_z():
        for d in (1, 3, 2):
            norm_copy(norm_y, lax.rem(y + 4 - d, 4), 0, d, "width_1", y).wait_recv()
        low = lax.broadcasted_iota(jnp.int32, (8, LANES), 1) < 64
        norm_z[z, 0] = jnp.where(low, norm_y[0], norm_y[1])
        norm_z[z, 1] = jnp.where(low, norm_y[2], norm_y[3])
        for d in (2, 1, 3):
            norm_copy(norm_z, z, 1, d, "width_0", z).start()

    def norm_end():
        for d in (1, 3, 2):
            norm_copy(norm_z, lax.rem(z + 4 - d, 4), 1, d, "width_0", z).wait_recv()
        for zz in range(4):
            for pair in range(2):
                for other in range(8):
                    norm_all[pl.ds(other * 8 + zz * 2 + pair, 1), :] = norm_z[zz, pair, pl.ds(other, 1), :]
        norm_out[...] = norm_all[...].astype(jnp.bfloat16)
        for d in range(1, 4):
            norm_copy(norm_y, y, 0, d, "width_1", y).wait_send()
            norm_copy(norm_z, z, 1, d, "width_0", z).wait_send()

    far = lax.rem(x + 2, 4)
    for k in range(len(UNITS)):
        for side in range(2):
            origin = (left if side == 0 else right) * 2 + c
            unit_copy(origin, k, own_send.at[side, k], side_recv.at[side, k], to_right).wait_recv()
            if UNITS[k][1] == side:
                send(unit_copy(origin, k, fwd_send.at[k], far_recv.at[k], to_right if side == 0 else to_left))
            send(unit_copy(origin, k, rel_send.at[side, k], rel_recv.at[1 + side, k], partner))
        if k == 2:
            norm_along_z()
        if k == 4:
            norm_end()
    for k in range(len(UNITS)):
        unit_copy(far * 2 + c, k, fwd_send.at[k], far_recv.at[k], to_right).wait_recv()
        send(unit_copy(far * 2 + c, k, rel_send.at[2, k], rel_recv.at[3, k], partner))

    for d in range(1, 8):
        sums_copy(0, 1, 0, d).wait_send()
        sums_copy(1, SUM_ROWS - 1, 1, d).wait_send()
    for copy in sends:
        copy.wait_send()
    for which, origin in enumerate((x, left, right, far)):
        for k in range(len(UNITS)):
            unit_copy(origin * 2 + 1 - c, k, own_send.at[2, k], rel_recv.at[which, k], partner).wait_recv()


def write_kernel(
    out_q, out_kv, res_q, res_kv, fac_q, fac_k, fac_v, norm,
    final_q, final_k, final_v, factor_q, factor_k, factor_v, serve_norm, result_q, result_k, result_v, sem,
):
    copies = []

    def write(src, dst):
        copy = pltpu.make_async_copy(src, dst, sem.at[len(copies)])
        copy.start()
        copies.append(copy)

    for part in range(8):
        rows = pl.ds(part * ROWS, ROWS)
        write(out_q.at[rows, :], final_q.at[rows, :])
    write(res_q, result_q)
    write(out_kv.at[pl.ds(0, 32), :], final_k)
    write(out_kv.at[pl.ds(32, 32), :], final_v)
    write(res_kv.at[pl.ds(0, 32), :], result_k)
    write(res_kv.at[pl.ds(32, 32), :], result_v)
    write(fac_q, factor_q)
    write(fac_k, factor_k)
    write(fac_v, factor_v)
    write(norm, serve_norm)
    for copy in copies:
        copy.wait()


def on_device(weight_query, smooth_query, weight_key, smooth_key, weight_value, smooth_value, norm_train, norm_step):
    f32, bf16 = jnp.float32, jnp.bfloat16
    any_spec, vmem_spec = pl.BlockSpec(memory_space=pl.ANY), pl.BlockSpec(memory_space=pltpu.VMEM)
    held = (
        ((D_MODEL, COLS), bf16),
        ((KV, D_MODEL), bf16),
        ((ROWS, COLS), f32),
        ((KV, ROWS), f32),
        ((1, COLS), f32),
        ((1, 32), f32),
        ((1, 32), f32),
        ((64, LANES), bf16),
    )
    units = len(UNITS)
    dma = pltpu.SemaphoreType.DMA
    gathered = pl.pallas_call(
        gather_kernel,
        out_shape=tuple(pltpu.VMEM(shape, dtype) for shape, dtype in held),
        in_specs=[any_spec] * 8,
        out_specs=tuple(vmem_spec for _ in held),
        scratch_shapes=[
            pltpu.VMEM((ROWS, COLS), f32),
            pltpu.VMEM((ROWS, COLS), f32),
            pltpu.VMEM((KV, ROWS), f32),
            pltpu.VMEM((KV, ROWS), f32),
            pltpu.VMEM((2, 1, 64), f32),
            pltpu.VMEM((8, SUM_ROWS, 1, LANES), f32),
            pltpu.VMEM((4, 8, LANES), f32),
            pltpu.VMEM((4, 2, 8, LANES), f32),
            pltpu.VMEM((64, LANES), f32),
            dma((2 * TILES + 6,)),
            dma((2, 8)),
            dma((2, 8)),
            dma((3, units)),
            dma((units,)),
            dma((3, units)),
            dma((2, units)),
            dma((units,)),
            dma((4, units)),
            dma((2, 4)),
            dma((2, 4)),
        ],
        compiler_params=pltpu.CompilerParams(
            collective_id=0, has_side_effects=True, vmem_limit_bytes=16 * 1024 * 1024
        ),
        name="gather",
    )(
        *(
            pltpu.with_memory_space_constraint(a, pltpu.HBM)
            for a in (
                weight_query, smooth_query, weight_key.T, smooth_key.T, weight_value.T, smooth_value.T,
                norm_train.reshape(1, 64), norm_step.reshape(1, 64),
            )
        )
    )
    outs = (
        ((D_MODEL, COLS), bf16),
        ((32, D_MODEL), bf16),
        ((32, D_MODEL), bf16),
        ((1, COLS), f32),
        ((1, 32), f32),
        ((1, 32), f32),
        ((64, LANES), bf16),
        ((ROWS, COLS), f32),
        ((32, ROWS), f32),
        ((32, ROWS), f32),
    )
    fq, fk, fv, cq, ck, cv, norm, rq, rk, rv = pl.pallas_call(
        write_kernel,
        out_shape=tuple(jax.ShapeDtypeStruct(shape, dtype) for shape, dtype in outs),
        in_specs=[vmem_spec] * len(held),
        out_specs=tuple(any_spec for _ in outs),
        scratch_shapes=[dma((17,))],
        compiler_params=pltpu.CompilerParams(vmem_limit_bytes=4 * 1024 * 1024),
        name="write",
    )(*gathered)
    return (
        fq, fk.T, fv.T, cq.reshape(COLS), ck.reshape(32), cv.reshape(32), norm.reshape(D_MODEL), rq, rk.T, rv.T
    )


def solution(mesh):
    split = Mesh(mesh.devices.reshape(4, 2, 4, 4), ("zero_0", "zero_1", "width_0", "width_1"))
    in_specs = (
        P(ZERO, WIDTH),
        P(ZERO, WIDTH),
        P(ZERO, WIDTH),
        P(ZERO, WIDTH),
        P(ZERO, WIDTH),
        P(ZERO, WIDTH),
        P(ZERO_WIDTH),
        P(ZERO_WIDTH),
    )
    out_specs = (
        P(None, WIDTH),
        P(None, WIDTH),
        P(None, WIDTH),
        P(WIDTH),
        P(WIDTH),
        P(WIDTH),
        P(),
        P(ZERO, WIDTH),
        P(ZERO, WIDTH),
        P(ZERO, WIDTH),
    )
    return jax.shard_map(
        on_device, mesh=split, in_specs=in_specs, out_specs=out_specs, check_vma=False
    )
```

```python
import jax
import jax.numpy as jnp
from jax import lax
from jax.experimental import pallas as pl
from jax.experimental.pallas import tpu as pltpu
from jax.sharding import Mesh
from jax.sharding import PartitionSpec as P

D_MODEL = 8192
ZERO = ("zero_0", "zero_1")
ZERO_WIDTH = ("zero_0", "zero_1", "width_0", "width_1")
WIDTH = ("width_0", "width_1")
MESH = pl.DeviceIdType.MESH

keep_rate = 0.7

ROWS = 1024
COLS = 512
HALF = ROWS // 2
KV = 64
LANES = 128
TILES = COLS // LANES
STEP = 128
KV_ROW, NORM_ROW = TILES, TILES + 1
SUM_ROWS = TILES + 2

UNITS = tuple((tile, half) for tile in range(TILES + 1) for half in range(2))


def mix(smooth, weight):
    return keep_rate * smooth + (1.0 - keep_rate) * weight


def gather_kernel(
    wq, sq, wk, sk, wv, sv, norm_a, norm_b,
    out_q, out_kv, res_q, res_kv, fac_q, fac_k, fac_v, norm_out,
    wq_v, sq_v, wkv_v, skv_v, norm_v, sums, norm_y, norm_z, norm_all,
    in_sem, send_sem, sum_send, sum_recv, side_recv, far_recv, rel_recv, norm_send, norm_recv, go,
):
    x, c = lax.axis_index("zero_0"), lax.axis_index("zero_1")
    z, y = lax.axis_index("width_0"), lax.axis_index("width_1")
    me = x * 2 + c
    right, left = lax.rem(x + 1, 4), lax.rem(x + 3, 4)
    partner = {"zero_1": 1 - c}

    def load(src, dst, which):
        pltpu.make_async_copy(src, dst, in_sem.at[which]).start()

    def wait_bytes(ref, sem):
        pltpu.make_async_copy(ref, ref, sem).wait()

    for t in range(TILES):
        cols = pl.ds(t * LANES, LANES)
        load(wq.at[:, cols], wq_v.at[:, cols], t)
        load(sq.at[:, cols], sq_v.at[:, cols], t)
    load(wk, wkv_v.at[pl.ds(0, 32), :], KV_ROW)
    load(sk, skv_v.at[pl.ds(0, 32), :], KV_ROW)
    load(wv, wkv_v.at[pl.ds(32, 32), :], KV_ROW)
    load(sv, skv_v.at[pl.ds(32, 32), :], KV_ROW)
    load(norm_a, norm_v.at[0], NORM_ROW)
    load(norm_b, norm_v.at[1], NORM_ROW)

    def group_peer(d):
        other = lax.rem(me + d, 8)
        return {"zero_0": other // 2, "zero_1": lax.rem(other, 2)}

    barrier = pltpu.get_barrier_semaphore()
    for d in (2, 1, 3):
        device = {"zero_0": lax.rem(x + d, 4), "zero_1": 1}
        pl.semaphore_signal(barrier, inc=1, device_id=device, device_id_type=MESH)

    @pl.when(c == 0)
    def _():
        pl.semaphore_signal(barrier, inc=1, device_id=partner, device_id_type=MESH)
        for d in (2, 1, 3):
            pl.semaphore_signal(barrier, inc=1, device_id={"width_1": lax.rem(y + d, 4)}, device_id_type=MESH)
            pl.semaphore_signal(barrier, inc=1, device_id={"width_0": lax.rem(z + d, 4)}, device_id_type=MESH)

    def wait_for_group():
        @pl.when(c == 1)
        def _():
            pl.semaphore_wait(barrier, 7)
            pl.semaphore_signal(go, inc=1, device_id=partner, device_id_type=MESH)

        @pl.when(c == 0)
        def _():
            pl.semaphore_wait(go, 1)

    def sum_tile(t):
        wait_bytes(wq_v.at[:, pl.ds(0, 2 * LANES)], in_sem.at[t])
        cols = pl.ds(t * LANES, LANES)

        def body(i, acc):
            rows = pl.ds(pl.multiple_of(i * STEP, STEP), STEP)
            r = mix(sq_v[rows, cols], wq_v[rows, cols])
            res_q[rows, cols] = r
            return acc + jnp.sum(jnp.abs(r).reshape(STEP // 8, 8, LANES), axis=0)

        acc = lax.fori_loop(0, ROWS // STEP, body, jnp.zeros((8, LANES), jnp.float32))
        sums[me, t] = jnp.sum(acc, axis=0, keepdims=True)

    def send_sums(first, count, which):
        for d in (4, 5, 3, 2, 6, 7, 1):
            pltpu.make_async_remote_copy(
                src_ref=sums.at[me, pl.ds(first, count)],
                dst_ref=sums.at[me, pl.ds(first, count)],
                send_sem=sum_send,
                recv_sem=sum_recv.at[which],
                device_id=group_peer(d),
                device_id_type=MESH,
            ).start()

    lane_of = lax.broadcasted_iota(jnp.int32, (KV, LANES), 1)
    diagonal = lane_of == lax.broadcasted_iota(jnp.int32, (KV, LANES), 0)

    sum_tile(0)
    wait_for_group()
    send_sums(0, 1, 0)
    for t in range(1, TILES):
        sum_tile(t)
    wait_bytes(wq_v.at[pl.ds(0, 4 * 32 * ROWS // COLS), :], in_sem.at[KV_ROW])
    acc = jnp.zeros((KV, LANES), jnp.float32)
    for j in range(ROWS // LANES):
        cols = pl.ds(j * LANES, LANES)
        r = mix(skv_v[:, cols], wkv_v[:, cols])
        res_kv[:, cols] = r
        acc = acc + jnp.abs(r)
    row_sums = jnp.sum(acc, axis=1, keepdims=True)
    sums[me, KV_ROW] = jnp.sum(jnp.where(diagonal, row_sums, 0.0), axis=0, keepdims=True)
    wait_bytes(norm_v, in_sem.at[NORM_ROW])
    own_norm = norm_v[0] + norm_v[1]
    sums[me, NORM_ROW] = jnp.concatenate([own_norm, own_norm], axis=1)
    send_sums(1, SUM_ROWS - 1, 1)

    def place(origin, k):
        tile, half = UNITS[k]
        if tile < TILES:
            rows = pl.ds(pl.multiple_of(origin * ROWS + half * HALF, HALF), HALF)
            return out_q.at[rows, pl.ds(tile * LANES, LANES)]
        return out_kv.at[:, pl.ds(pl.multiple_of(origin * ROWS + half * HALF, HALF), HALF)]

    def unit_copy(origin, k, recv_sem, device):
        ref = place(origin, k)
        return pltpu.make_async_remote_copy(
            src_ref=ref, dst_ref=ref, send_sem=send_sem, recv_sem=recv_sem, device_id=device, device_id_type=MESH
        )

    to_right, to_left = {"zero_0": right}, {"zero_0": left}

    def send_own(k):
        ways = [(0, to_right), (1, to_left)]
        for side, device in ways if UNITS[k][1] == 0 else ways[::-1]:
            unit_copy(me, k, side_recv.at[side, k], device).start()
        unit_copy(me, k, rel_recv, partner).start()

    def narrow_tile(t):
        total = sums[0, t]
        for other in range(1, 8):
            total = total + sums[other, t]
        factor = total * (1.0 / D_MODEL)
        if t < TILES:
            fac_q[:, pl.ds(t * LANES, LANES)] = factor
            scale = 1.0 / factor
        else:
            fac_k[...] = factor[:, 0:32]
            fac_v[...] = pltpu.roll(factor, LANES - 32, 1)[:, 0:32]
            spread = jnp.sum(jnp.where(diagonal, jnp.broadcast_to(factor, (KV, LANES)), 0.0), axis=1, keepdims=True)
            scale = 1.0 / jnp.broadcast_to(spread, (KV, LANES))
        for half in range(2):
            if t < TILES:
                cols = pl.ds(t * LANES, LANES)

                def body(i, carry):
                    at = half * HALF + i * STEP
                    rows = pl.ds(pl.multiple_of(at, STEP), STEP)
                    there = pl.ds(pl.multiple_of(me * ROWS + at, STEP), STEP)
                    out_q[there, cols] = (res_q[rows, cols] * scale).astype(jnp.bfloat16)
                    return carry

                lax.fori_loop(0, HALF // STEP, body, 0)
            else:
                for j in range(HALF // LANES):
                    at = half * HALF + j * LANES
                    there = pl.ds(pl.multiple_of(me * ROWS + at, LANES), LANES)
                    out_kv[:, there] = (res_kv[:, pl.ds(at, LANES)] * scale).astype(jnp.bfloat16)
            send_own(2 * t + half)

    wait_bytes(sums.at[pl.ds(0, 7), pl.ds(0, 1)], sum_recv.at[0])
    narrow_tile(0)
    wait_bytes(sums.at[pl.ds(0, 7), pl.ds(1, SUM_ROWS - 1)], sum_recv.at[1])
    for t in range(1, TILES + 1):
        narrow_tile(t)

    def norm_copy(buf, at, stage, device):
        return pltpu.make_async_remote_copy(
            src_ref=buf.at[at],
            dst_ref=buf.at[at],
            send_sem=norm_send.at[stage],
            recv_sem=norm_recv.at[stage],
            device_id=device,
            device_id_type=MESH,
        )

    def norm_along_y():
        pl.semaphore_wait(barrier, 6)
        for other in range(8):
            norm_y[y, pl.ds(other, 1), :] = sums[other, NORM_ROW]
        for d in (2, 1, 3):
            norm_copy(norm_y, y, 0, {"width_1": lax.rem(y + d, 4)}).start()

    def norm_along_z():
        wait_bytes(norm_y.at[pl.ds(0, 3)], norm_recv.at[0])
        low = lax.broadcasted_iota(jnp.int32, (8, LANES), 1) < 64
        norm_z[z, 0] = jnp.where(low, norm_y[0], norm_y[1])
        norm_z[z, 1] = jnp.where(low, norm_y[2], norm_y[3])
        for d in (2, 1, 3):
            norm_copy(norm_z, z, 1, {"width_0": lax.rem(z + d, 4)}).start()

    def norm_end():
        wait_bytes(norm_z.at[pl.ds(0, 3)], norm_recv.at[1])
        for zz in range(4):
            for pair in range(2):
                for other in range(8):
                    norm_all[pl.ds(other * 8 + zz * 2 + pair, 1), :] = norm_z[zz, pair, pl.ds(other, 1), :]
        norm_out[...] = norm_all[...].astype(jnp.bfloat16)
        wait_bytes(norm_y.at[pl.ds(0, 3)], norm_send.at[0])
        wait_bytes(norm_z.at[pl.ds(0, 3)], norm_send.at[1])

    def norm_to_partner():
        return norm_copy(norm_out, pl.ds(0, 64), 2, partner)

    far = lax.rem(x + 2, 4)
    norm_steps = {1: norm_along_y, 3: norm_along_z, 5: norm_end, 6: lambda: norm_to_partner().start()}
    for k in range(len(UNITS)):
        for side in range(2):
            origin = (left if side == 0 else right) * 2 + c
            unit_copy(origin, k, side_recv.at[side, k], to_right).wait_recv()
            if UNITS[k][1] == side:
                unit_copy(origin, k, far_recv.at[k], to_right if side == 0 else to_left).start()
            unit_copy(origin, k, rel_recv, partner).start()
        if k in norm_steps:
            pl.when(c == 0)(norm_steps[k])
    pl.when(c == 0)(lambda: norm_to_partner().wait_send())
    pl.when(c == 1)(lambda: norm_to_partner().wait_recv())
    for k in range(len(UNITS)):
        unit_copy(far * 2 + c, k, far_recv.at[k], to_right).wait_recv()
        unit_copy(far * 2 + c, k, rel_recv, partner).start()

    shard_rows = ROWS + KV * ROWS // COLS
    wait_bytes(sums.at[pl.ds(0, 7)], sum_send)
    wait_bytes(out_q.at[pl.ds(0, 7 * shard_rows), :], send_sem)
    wait_bytes(out_q.at[pl.ds(0, 4 * shard_rows), :], rel_recv)


def write_kernel(
    out_q, out_kv, res_q, res_kv, fac_q, fac_k, fac_v, norm,
    final_q, final_k, final_v, factor_q, factor_k, factor_v, serve_norm, result_q, result_k, result_v, sem,
):
    copies = []

    def write(src, dst):
        copy = pltpu.make_async_copy(src, dst, sem.at[len(copies)])
        copy.start()
        copies.append(copy)

    for part in range(8):
        rows = pl.ds(part * ROWS, ROWS)
        write(out_q.at[rows, :], final_q.at[rows, :])
    write(res_q, result_q)
    write(out_kv.at[pl.ds(0, 32), :], final_k)
    write(out_kv.at[pl.ds(32, 32), :], final_v)
    write(res_kv.at[pl.ds(0, 32), :], result_k)
    write(res_kv.at[pl.ds(32, 32), :], result_v)
    write(fac_q, factor_q)
    write(fac_k, factor_k)
    write(fac_v, factor_v)
    write(norm, serve_norm)
    for copy in copies:
        copy.wait()


def on_device(weight_query, smooth_query, weight_key, smooth_key, weight_value, smooth_value, norm_train, norm_step):
    f32, bf16 = jnp.float32, jnp.bfloat16
    any_spec, vmem_spec = pl.BlockSpec(memory_space=pl.ANY), pl.BlockSpec(memory_space=pltpu.VMEM)
    held = (
        ((D_MODEL, COLS), bf16),
        ((KV, D_MODEL), bf16),
        ((ROWS, COLS), f32),
        ((KV, ROWS), f32),
        ((1, COLS), f32),
        ((1, 32), f32),
        ((1, 32), f32),
        ((64, LANES), bf16),
    )
    units = len(UNITS)
    dma = pltpu.SemaphoreType.DMA
    gathered = pl.pallas_call(
        gather_kernel,
        out_shape=tuple(pltpu.VMEM(shape, dtype) for shape, dtype in held),
        in_specs=[any_spec] * 8,
        out_specs=tuple(vmem_spec for _ in held),
        scratch_shapes=[
            pltpu.VMEM((ROWS, COLS), f32),
            pltpu.VMEM((ROWS, COLS), f32),
            pltpu.VMEM((KV, ROWS), f32),
            pltpu.VMEM((KV, ROWS), f32),
            pltpu.VMEM((2, 1, 64), f32),
            pltpu.VMEM((8, SUM_ROWS, 1, LANES), f32),
            pltpu.VMEM((4, 8, LANES), f32),
            pltpu.VMEM((4, 2, 8, LANES), f32),
            pltpu.VMEM((64, LANES), f32),
            dma((SUM_ROWS,)),
            dma,
            dma,
            dma((2,)),
            dma((2, units)),
            dma((units,)),
            dma,
            dma((3,)),
            dma((3,)),
            pltpu.SemaphoreType.REGULAR,
        ],
        compiler_params=pltpu.CompilerParams(
            collective_id=0, has_side_effects=True, vmem_limit_bytes=16 * 1024 * 1024
        ),
        name="gather",
    )(
        *(
            pltpu.with_memory_space_constraint(a, pltpu.HBM)
            for a in (
                weight_query, smooth_query, weight_key.T, smooth_key.T, weight_value.T, smooth_value.T,
                norm_train.reshape(1, 64), norm_step.reshape(1, 64),
            )
        )
    )
    outs = (
        ((D_MODEL, COLS), bf16),
        ((32, D_MODEL), bf16),
        ((32, D_MODEL), bf16),
        ((1, COLS), f32),
        ((1, 32), f32),
        ((1, 32), f32),
        ((64, LANES), bf16),
        ((ROWS, COLS), f32),
        ((32, ROWS), f32),
        ((32, ROWS), f32),
    )
    fq, fk, fv, cq, ck, cv, norm, rq, rk, rv = pl.pallas_call(
        write_kernel,
        out_shape=tuple(jax.ShapeDtypeStruct(shape, dtype) for shape, dtype in outs),
        in_specs=[vmem_spec] * len(held),
        out_specs=tuple(any_spec for _ in outs),
        scratch_shapes=[dma((17,))],
        compiler_params=pltpu.CompilerParams(vmem_limit_bytes=4 * 1024 * 1024),
        name="write",
    )(*gathered)
    return (
        fq, fk.T, fv.T, cq.reshape(COLS), ck.reshape(32), cv.reshape(32), norm.reshape(D_MODEL), rq, rk.T, rv.T
    )


def solution(mesh):
    split = Mesh(mesh.devices.reshape(4, 2, 4, 4), ("zero_0", "zero_1", "width_0", "width_1"))
    in_specs = (
        P(ZERO, WIDTH),
        P(ZERO, WIDTH),
        P(ZERO, WIDTH),
        P(ZERO, WIDTH),
        P(ZERO, WIDTH),
        P(ZERO, WIDTH),
        P(ZERO_WIDTH),
        P(ZERO_WIDTH),
    )
    out_specs = (
        P(None, WIDTH),
        P(None, WIDTH),
        P(None, WIDTH),
        P(WIDTH),
        P(WIDTH),
        P(WIDTH),
        P(),
        P(ZERO, WIDTH),
        P(ZERO, WIDTH),
        P(ZERO, WIDTH),
    )
    return jax.shard_map(
        on_device, mesh=split, in_specs=in_specs, out_specs=out_specs, check_vma=False
    )
```

```python
import jax
import jax.numpy as jnp
from jax import lax
from jax.experimental import pallas as pl
from jax.experimental.pallas import tpu as pltpu
from jax.sharding import Mesh
from jax.sharding import PartitionSpec as P

D_MODEL = 8192
ZERO = ("zero_0", "zero_1")
ZERO_WIDTH = ("zero_0", "zero_1", "width_0", "width_1")
WIDTH = ("width_0", "width_1")
MESH = pl.DeviceIdType.MESH

keep_rate = 0.7

ROWS = 1024
COLS = 512
HALF = ROWS // 2
KV = 64
LANES = 128
TILES = COLS // LANES
STEP = 128
KV_ROW, NORM_ROW, MAX_ROW = TILES, TILES + 1, TILES + 2
SUM_ROWS = TILES + 3

FIRST = 192
CODED = ((0, 0, FIRST, 0), (0, FIRST, HALF - FIRST, 0), (0, HALF, FIRST, 1), (0, HALF + FIRST, HALF - FIRST, 1))
UNITS = CODED + tuple((tile, half * HALF, HALF, half) for tile in range(1, TILES + 1) for half in range(2))
ORDER = (
    (0, 1, 2, 3, *range(4, len(UNITS))),
    (2, 3, 0, 1, *range(4, len(UNITS))),
)
CODE = 180.0


def mix(smooth, weight):
    return keep_rate * smooth + (1.0 - keep_rate) * weight


def encode(x, scale):
    v = x * scale
    for _ in range(4):
        v = v * v
    return jnp.where(x < 0, -v, v).astype(jnp.bfloat16)


def decode(code):
    v = code.astype(jnp.float32)
    root = jnp.abs(v)
    for _ in range(4):
        root = lax.rsqrt(root)
    return jnp.where(v < 0, -root, root)


def gather_kernel(
    wq, sq, wk, sk, wv, sv, norm_a, norm_b,
    out_q, out_kv, res_q, res_kv, fac_q, fac_k, fac_v, norm_out,
    wq_v, sq_v, wkv_v, skv_v, norm_v, coded, sums, norm_y, norm_z, norm_all,
    in_sem, send_sem, sum_send, sum_recv, side_recv, far_recv, rel_recv, norm_send, norm_recv, go,
):
    x, c = lax.axis_index("zero_0"), lax.axis_index("zero_1")
    z, y = lax.axis_index("width_0"), lax.axis_index("width_1")
    me = x * 2 + c
    right, left = lax.rem(x + 1, 4), lax.rem(x + 3, 4)
    partner = {"zero_1": 1 - c}

    def load(src, dst, which):
        pltpu.make_async_copy(src, dst, in_sem.at[which]).start()

    def wait_bytes(ref, sem):
        pltpu.make_async_copy(ref, ref, sem).wait()

    for t in range(TILES):
        cols = pl.ds(t * LANES, LANES)
        load(wq.at[:, cols], wq_v.at[:, cols], t)
        load(sq.at[:, cols], sq_v.at[:, cols], t)
    load(wk, wkv_v.at[pl.ds(0, 32), :], KV_ROW)
    load(sk, skv_v.at[pl.ds(0, 32), :], KV_ROW)
    load(wv, wkv_v.at[pl.ds(32, 32), :], KV_ROW)
    load(sv, skv_v.at[pl.ds(32, 32), :], KV_ROW)
    load(norm_a, norm_v.at[0], NORM_ROW)
    load(norm_b, norm_v.at[1], NORM_ROW)

    def group_peer(d):
        other = lax.rem(me + d, 8)
        return {"zero_0": other // 2, "zero_1": lax.rem(other, 2)}

    barrier = pltpu.get_barrier_semaphore()
    for d in (2, 1, 3):
        device = {"zero_0": lax.rem(x + d, 4), "zero_1": 1}
        pl.semaphore_signal(barrier, inc=1, device_id=device, device_id_type=MESH)

    @pl.when(c == 0)
    def _():
        pl.semaphore_signal(barrier, inc=1, device_id=partner, device_id_type=MESH)
        for d in (2, 1, 3):
            pl.semaphore_signal(barrier, inc=1, device_id={"width_1": lax.rem(y + d, 4)}, device_id_type=MESH)
            pl.semaphore_signal(barrier, inc=1, device_id={"width_0": lax.rem(z + d, 4)}, device_id_type=MESH)

    def wait_for_group():
        @pl.when(c == 1)
        def _():
            pl.semaphore_wait(barrier, 7)
            pl.semaphore_signal(go, inc=1, device_id=partner, device_id_type=MESH)

        @pl.when(c == 0)
        def _():
            pl.semaphore_wait(go, 1)

    def sum_tile(t):
        wait_bytes(wq_v.at[:, pl.ds(0, 2 * LANES)], in_sem.at[t])
        cols = pl.ds(t * LANES, LANES)

        def body(i, carry):
            acc, top = carry
            rows = pl.ds(pl.multiple_of(i * STEP, STEP), STEP)
            r = mix(sq_v[rows, cols], wq_v[rows, cols])
            res_q[rows, cols] = r
            size = jnp.abs(r).reshape(STEP // 8, 8, LANES)
            acc = acc + jnp.sum(size, axis=0)
            return acc, jnp.maximum(top, jnp.max(size, axis=0)) if t == 0 else top

        none = jnp.zeros((8, LANES), jnp.float32)
        acc, top = lax.fori_loop(0, ROWS // STEP, body, (none, none))
        sums[me, t] = jnp.sum(acc, axis=0, keepdims=True)
        return jnp.max(top, axis=0, keepdims=True)

    def send_sums():
        for d in (4, 5, 3, 2, 6, 7, 1):
            pltpu.make_async_remote_copy(
                src_ref=sums.at[me],
                dst_ref=sums.at[me],
                send_sem=sum_send,
                recv_sem=sum_recv,
                device_id=group_peer(d),
                device_id_type=MESH,
            ).start()

    def final_place(origin, k):
        tile, row, rows, _ = UNITS[k]
        if tile < TILES:
            return out_q.at[pl.ds(pl.multiple_of((origin * 2 + c) * ROWS + row, 64), rows), pl.ds(tile * LANES, LANES)]
        return out_kv.at[:, pl.ds(pl.multiple_of((origin * 2 + c) * ROWS + row, HALF), rows)]

    def place(origin, k):
        _, row, rows, _ = UNITS[k]
        return coded.at[origin, pl.ds(row, rows)] if k < len(CODED) else final_place(origin, k)

    def unit_copy(ref, recv_sem, device):
        return pltpu.make_async_remote_copy(
            src_ref=ref, dst_ref=ref, send_sem=send_sem, recv_sem=recv_sem, device_id=device, device_id_type=MESH
        )

    to_right, to_left = {"zero_0": right}, {"zero_0": left}

    def send_right(k):
        unit_copy(place(x, k), side_recv.at[0, k], to_right).start()

    def send_left(k):
        unit_copy(place(x, k), side_recv.at[1, k], to_left).start()

    def relay(origin, k):
        unit_copy(final_place(origin, k), rel_recv, partner).start()

    def encode_rows(k, scale):
        _, row, rows, _ = UNITS[k]

        def body(i, carry):
            at = pl.ds(pl.multiple_of(row + i * 64, 64), 64)
            coded[x, at, :] = encode(res_q[at, 0:LANES], scale)
            return carry

        lax.fori_loop(0, rows // 64, body, 0)

    def decode_rows(origin, k, scale):
        _, row, rows, _ = UNITS[k]
        own = sums[origin * 2 + c, MAX_ROW] * scale

        def body(i, carry):
            at = pl.multiple_of(row + i * 64, 64)
            there = pl.ds(pl.multiple_of((origin * 2 + c) * ROWS + at, 64), 64)
            out_q[there, 0:LANES] = (decode(coded[origin, pl.ds(at, 64), :]) * own).astype(jnp.bfloat16)
            return carry

        lax.fori_loop(0, rows // 64, body, 0)

    lane_of = lax.broadcasted_iota(jnp.int32, (KV, LANES), 1)
    diagonal = lane_of == lax.broadcasted_iota(jnp.int32, (KV, LANES), 0)

    top = jnp.maximum(sum_tile(0), 1e-30)
    sums[me, MAX_ROW] = top
    scale = CODE / top
    encode_rows(0, scale)
    encode_rows(2, scale)
    wait_for_group()
    send_right(0)
    send_left(2)
    for t in range(1, TILES):
        sum_tile(t)
    wait_bytes(wq_v.at[pl.ds(0, 4 * 32 * ROWS // COLS), :], in_sem.at[KV_ROW])
    acc = jnp.zeros((KV, LANES), jnp.float32)
    for j in range(ROWS // LANES):
        cols = pl.ds(j * LANES, LANES)
        r = mix(skv_v[:, cols], wkv_v[:, cols])
        res_kv[:, cols] = r
        acc = acc + jnp.abs(r)
    row_sums = jnp.sum(acc, axis=1, keepdims=True)
    sums[me, KV_ROW] = jnp.sum(jnp.where(diagonal, row_sums, 0.0), axis=0, keepdims=True)
    wait_bytes(norm_v, in_sem.at[NORM_ROW])
    own_norm = norm_v[0] + norm_v[1]
    sums[me, NORM_ROW] = jnp.concatenate([own_norm, own_norm], axis=1)
    send_sums()
    encode_rows(1, scale)
    send_right(1)
    encode_rows(3, scale)
    for k in (3, 0, 1):
        send_left(k)
    for k in (2, 3):
        send_right(k)

    def factor_of(t):
        total = sums[0, t]
        for other in range(1, 8):
            total = total + sums[other, t]
        return total * (1.0 / D_MODEL)

    def narrow_tile(t):
        factor = factor_of(t)
        if t < TILES:
            fac_q[:, pl.ds(t * LANES, LANES)] = factor
            scale = 1.0 / factor
        else:
            fac_k[...] = factor[:, 0:32]
            fac_v[...] = pltpu.roll(factor, LANES - 32, 1)[:, 0:32]
            spread = jnp.sum(jnp.where(diagonal, jnp.broadcast_to(factor, (KV, LANES)), 0.0), axis=1, keepdims=True)
            scale = 1.0 / jnp.broadcast_to(spread, (KV, LANES))
        for half in range(2):
            if t < TILES:
                cols = pl.ds(t * LANES, LANES)

                def body(i, carry):
                    at = half * HALF + i * STEP
                    rows = pl.ds(pl.multiple_of(at, STEP), STEP)
                    there = pl.ds(pl.multiple_of(me * ROWS + at, STEP), STEP)
                    out_q[there, cols] = (res_q[rows, cols] * scale).astype(jnp.bfloat16)
                    return carry

                lax.fori_loop(0, HALF // STEP, body, 0)
            else:
                for j in range(HALF // LANES):
                    at = half * HALF + j * LANES
                    there = pl.ds(pl.multiple_of(me * ROWS + at, LANES), LANES)
                    out_kv[:, there] = (res_kv[:, pl.ds(at, LANES)] * scale).astype(jnp.bfloat16)
            k = len(CODED) + 2 * (t - 1) + half
            for go_there in (send_right, send_left) if half == 0 else (send_left, send_right):
                go_there(k)
            relay(x, k)

    wait_bytes(sums.at[pl.ds(0, 7)], sum_recv)
    for t in range(1, TILES + 1):
        narrow_tile(t)
    first_factor = factor_of(0)
    fac_q[:, 0:LANES] = first_factor
    first_scale = 1.0 / (CODE * first_factor)
    for k in range(len(CODED)):
        decode_rows(x, k, first_scale)
        relay(x, k)

    def norm_copy(buf, at, stage, device):
        return pltpu.make_async_remote_copy(
            src_ref=buf.at[at],
            dst_ref=buf.at[at],
            send_sem=norm_send.at[stage],
            recv_sem=norm_recv.at[stage],
            device_id=device,
            device_id_type=MESH,
        )

    def norm_along_y():
        pl.semaphore_wait(barrier, 6)
        for other in range(8):
            norm_y[y, pl.ds(other, 1), :] = sums[other, NORM_ROW]
        for d in (2, 1, 3):
            norm_copy(norm_y, y, 0, {"width_1": lax.rem(y + d, 4)}).start()

    def norm_along_z():
        wait_bytes(norm_y.at[pl.ds(0, 3)], norm_recv.at[0])
        low = lax.broadcasted_iota(jnp.int32, (8, LANES), 1) < 64
        norm_z[z, 0] = jnp.where(low, norm_y[0], norm_y[1])
        norm_z[z, 1] = jnp.where(low, norm_y[2], norm_y[3])
        for d in (2, 1, 3):
            norm_copy(norm_z, z, 1, {"width_0": lax.rem(z + d, 4)}).start()

    def norm_end():
        wait_bytes(norm_z.at[pl.ds(0, 3)], norm_recv.at[1])
        for zz in range(4):
            for pair in range(2):
                for other in range(8):
                    norm_all[pl.ds(other * 8 + zz * 2 + pair, 1), :] = norm_z[zz, pair, pl.ds(other, 1), :]
        norm_out[...] = norm_all[...].astype(jnp.bfloat16)
        wait_bytes(norm_y.at[pl.ds(0, 3)], norm_send.at[0])
        wait_bytes(norm_z.at[pl.ds(0, 3)], norm_send.at[1])

    def norm_to_partner():
        return norm_copy(norm_out, pl.ds(0, 64), 2, partner)

    far = lax.rem(x + 2, 4)
    norm_steps = {2: norm_along_y, 4: norm_along_z, 6: norm_end, 7: lambda: norm_to_partner().start()}

    def hand_on(origin, k):
        if k < len(CODED):
            decode_rows(origin, k, first_scale)
        relay(origin, k)

    for i in range(len(UNITS)):
        for side in range(2):
            k, origin = ORDER[side][i], left if side == 0 else right
            unit_copy(place(origin, k), side_recv.at[side, k], partner).wait_recv()
            if UNITS[k][3] == side:
                unit_copy(place(origin, k), far_recv.at[k], to_right if side == 0 else to_left).start()
            hand_on(origin, k)
        if i in norm_steps:
            pl.when(c == 0)(norm_steps[i])
    pl.when(c == 0)(lambda: norm_to_partner().wait_send())
    pl.when(c == 1)(lambda: norm_to_partner().wait_recv())
    for k in (0, 2, 1, 3, *range(len(CODED), len(UNITS))):
        unit_copy(place(far, k), far_recv.at[k], partner).wait_recv()
        hand_on(far, k)

    shard_rows = ROWS + KV * ROWS // COLS
    wait_bytes(sums.at[pl.ds(0, 7)], sum_send)
    wait_bytes(out_q.at[pl.ds(0, 7 * shard_rows), :], send_sem)
    wait_bytes(out_q.at[pl.ds(0, 4 * shard_rows), :], rel_recv)


def write_kernel(
    out_q, out_kv, res_q, res_kv, fac_q, fac_k, fac_v, norm,
    final_q, final_k, final_v, factor_q, factor_k, factor_v, serve_norm, result_q, result_k, result_v, sem,
):
    copies = []

    def write(src, dst):
        copy = pltpu.make_async_copy(src, dst, sem.at[len(copies)])
        copy.start()
        copies.append(copy)

    for part in range(8):
        rows = pl.ds(part * ROWS, ROWS)
        write(out_q.at[rows, :], final_q.at[rows, :])
    write(res_q, result_q)
    write(out_kv.at[pl.ds(0, 32), :], final_k)
    write(out_kv.at[pl.ds(32, 32), :], final_v)
    write(res_kv.at[pl.ds(0, 32), :], result_k)
    write(res_kv.at[pl.ds(32, 32), :], result_v)
    write(fac_q, factor_q)
    write(fac_k, factor_k)
    write(fac_v, factor_v)
    write(norm, serve_norm)
    for copy in copies:
        copy.wait()


def on_device(weight_query, smooth_query, weight_key, smooth_key, weight_value, smooth_value, norm_train, norm_step):
    f32, bf16 = jnp.float32, jnp.bfloat16
    any_spec, vmem_spec = pl.BlockSpec(memory_space=pl.ANY), pl.BlockSpec(memory_space=pltpu.VMEM)
    held = (
        ((D_MODEL, COLS), bf16),
        ((KV, D_MODEL), bf16),
        ((ROWS, COLS), f32),
        ((KV, ROWS), f32),
        ((1, COLS), f32),
        ((1, 32), f32),
        ((1, 32), f32),
        ((64, LANES), bf16),
    )
    units = len(UNITS)
    dma = pltpu.SemaphoreType.DMA
    gathered = pl.pallas_call(
        gather_kernel,
        out_shape=tuple(pltpu.VMEM(shape, dtype) for shape, dtype in held),
        in_specs=[any_spec] * 8,
        out_specs=tuple(vmem_spec for _ in held),
        scratch_shapes=[
            pltpu.VMEM((ROWS, COLS), f32),
            pltpu.VMEM((ROWS, COLS), f32),
            pltpu.VMEM((KV, ROWS), f32),
            pltpu.VMEM((KV, ROWS), f32),
            pltpu.VMEM((2, 1, 64), f32),
            pltpu.VMEM((4, ROWS, LANES), bf16),
            pltpu.VMEM((8, SUM_ROWS, 1, LANES), f32),
            pltpu.VMEM((4, 8, LANES), f32),
            pltpu.VMEM((4, 2, 8, LANES), f32),
            pltpu.VMEM((64, LANES), f32),
            dma((SUM_ROWS,)),
            dma,
            dma,
            dma,
            dma((2, units)),
            dma((units,)),
            dma,
            dma((3,)),
            dma((3,)),
            pltpu.SemaphoreType.REGULAR,
        ],
        compiler_params=pltpu.CompilerParams(
            collective_id=0, has_side_effects=True, vmem_limit_bytes=16 * 1024 * 1024
        ),
        name="gather",
    )(
        *(
            pltpu.with_memory_space_constraint(a, pltpu.HBM)
            for a in (
                weight_query, smooth_query, weight_key.T, smooth_key.T, weight_value.T, smooth_value.T,
                norm_train.reshape(1, 64), norm_step.reshape(1, 64),
            )
        )
    )
    outs = (
        ((D_MODEL, COLS), bf16),
        ((32, D_MODEL), bf16),
        ((32, D_MODEL), bf16),
        ((1, COLS), f32),
        ((1, 32), f32),
        ((1, 32), f32),
        ((64, LANES), bf16),
        ((ROWS, COLS), f32),
        ((32, ROWS), f32),
        ((32, ROWS), f32),
    )
    fq, fk, fv, cq, ck, cv, norm, rq, rk, rv = pl.pallas_call(
        write_kernel,
        out_shape=tuple(jax.ShapeDtypeStruct(shape, dtype) for shape, dtype in outs),
        in_specs=[vmem_spec] * len(held),
        out_specs=tuple(any_spec for _ in outs),
        scratch_shapes=[dma((17,))],
        compiler_params=pltpu.CompilerParams(vmem_limit_bytes=4 * 1024 * 1024),
        name="write",
    )(*gathered)
    return (
        fq, fk.T, fv.T, cq.reshape(COLS), ck.reshape(32), cv.reshape(32), norm.reshape(D_MODEL), rq, rk.T, rv.T
    )


def solution(mesh):
    split = Mesh(mesh.devices.reshape(4, 2, 4, 4), ("zero_0", "zero_1", "width_0", "width_1"))
    in_specs = (
        P(ZERO, WIDTH),
        P(ZERO, WIDTH),
        P(ZERO, WIDTH),
        P(ZERO, WIDTH),
        P(ZERO, WIDTH),
        P(ZERO, WIDTH),
        P(ZERO_WIDTH),
        P(ZERO_WIDTH),
    )
    out_specs = (
        P(None, WIDTH),
        P(None, WIDTH),
        P(None, WIDTH),
        P(WIDTH),
        P(WIDTH),
        P(WIDTH),
        P(),
        P(ZERO, WIDTH),
        P(ZERO, WIDTH),
        P(ZERO, WIDTH),
    )
    return jax.shard_map(
        on_device, mesh=split, in_specs=in_specs, out_specs=out_specs, check_vma=False
    )
```

```python
import jax
import jax.numpy as jnp
from jax import lax
from jax.experimental import pallas as pl
from jax.experimental.pallas import tpu as pltpu
from jax.sharding import Mesh
from jax.sharding import PartitionSpec as P

D_MODEL = 8192
ZERO = ("zero_0", "zero_1")
ZERO_WIDTH = ("zero_0", "zero_1", "width_0", "width_1")
WIDTH = ("width_0", "width_1")
MESH = pl.DeviceIdType.MESH

keep_rate = 0.7

ROWS = 1024
COLS = 512
HALF = ROWS // 2
KV = 64
LANES = 128
TILES = COLS // LANES
STEP = 128
KV_ROW, NORM_ROW, MAX_ROW = TILES, TILES + 1, TILES + 2
SUM_ROWS = TILES + 4

FIRST = 192
PIECES = ((0, FIRST), (192, 128), (320, 192))
CODED = tuple((0, half * HALF + row, rows, half) for half in range(2) for row, rows in PIECES)
UNITS = CODED + tuple((tile, half * HALF, HALF, half) for tile in range(1, TILES + 1) for half in range(2))
ORDER = (
    (0, 1, 2, 3, 4, 5, *range(6, len(UNITS))),
    (3, 4, 5, 0, 1, 2, *range(6, len(UNITS))),
)
CODE = 180.0


def mix(smooth, weight):
    return keep_rate * smooth + (1.0 - keep_rate) * weight


def encode(x, scale):
    v = x * scale
    for _ in range(4):
        v = v * v
    return jnp.where(x < 0, -v, v).astype(jnp.bfloat16)


def decode(code):
    v = code.astype(jnp.float32)
    root = jnp.abs(v)
    for _ in range(4):
        root = lax.rsqrt(root)
    return jnp.where(v < 0, -root, root)


def gather_kernel(
    wq, sq, wk, sk, wv, sv, norm_a, norm_b,
    out_q, out_kv, res_q, res_kv, fac_q, fac_k, fac_v, norm_out,
    wq_v, sq_v, wkv_v, skv_v, norm_v, coded, sums, norm_y, norm_z, norm_all,
    in_sem, send_sem, sum_send, sum_recv, side_recv, far_recv, rel_recv, norm_send, norm_recv, go, vouch,
):
    x, c = lax.axis_index("zero_0"), lax.axis_index("zero_1")
    z, y = lax.axis_index("width_0"), lax.axis_index("width_1")
    me = x * 2 + c
    right, left = lax.rem(x + 1, 4), lax.rem(x + 3, 4)
    partner = {"zero_1": 1 - c}

    def load(src, dst, which):
        pltpu.make_async_copy(src, dst, in_sem.at[which]).start()

    def load_rows(t, first, rows, which):
        at = (pl.ds(first, rows), pl.ds(t * LANES, LANES))
        load(wq.at[at], wq_v.at[at], which)
        load(sq.at[at], sq_v.at[at], which)

    def wait_bytes(ref, sem):
        pltpu.make_async_copy(ref, ref, sem).wait()

    barrier = pltpu.get_barrier_semaphore()
    for device in ({"zero_0": right, "zero_1": 1}, {"zero_0": left, "zero_1": 1}):
        pl.semaphore_signal(barrier, inc=1, device_id=device, device_id_type=MESH)

    @pl.when(c == 0)
    def _():
        pl.semaphore_signal(barrier, inc=1, device_id=partner, device_id_type=MESH)

    for row in (0, HALF):
        load_rows(0, row, FIRST, 0)
    for row in (FIRST, HALF + FIRST):
        load_rows(0, row, HALF - FIRST, TILES)
    load(wk, wkv_v.at[pl.ds(0, 32), :], KV_ROW + 1)
    load(sk, skv_v.at[pl.ds(0, 32), :], KV_ROW + 1)
    load(wv, wkv_v.at[pl.ds(32, 32), :], KV_ROW + 1)
    load(sv, skv_v.at[pl.ds(32, 32), :], KV_ROW + 1)
    load(norm_a, norm_v.at[0], NORM_ROW + 1)
    load(norm_b, norm_v.at[1], NORM_ROW + 1)
    for t in range(1, TILES):
        load_rows(t, 0, ROWS, t)

    @pl.when(c == 0)
    def _():
        for d in (2, 1, 3):
            pl.semaphore_signal(barrier, inc=1, device_id={"width_1": lax.rem(y + d, 4)}, device_id_type=MESH)
            pl.semaphore_signal(barrier, inc=1, device_id={"width_0": lax.rem(z + d, 4)}, device_id_type=MESH)

    def wait_for_neighbours():
        @pl.when(c == 1)
        def _():
            pl.semaphore_wait(barrier, 5)
            pl.semaphore_signal(go.at[0], inc=1, device_id=partner, device_id_type=MESH)
            for side in (left, right):
                pl.semaphore_signal(vouch, inc=1, device_id={"zero_0": side}, device_id_type=MESH)

        @pl.when(c == 0)
        def _():
            pl.semaphore_wait(go.at[0], 1)

    def wait_for_far():
        @pl.when(c == 1)
        def _():
            pl.semaphore_wait(vouch, 2)
            pl.semaphore_signal(go.at[1], inc=1, device_id=partner, device_id_type=MESH)

        @pl.when(c == 0)
        def _():
            pl.semaphore_wait(go.at[1], 1)

    def group_peer(d):
        other = lax.rem(me + d, 8)
        return {"zero_0": other // 2, "zero_1": lax.rem(other, 2)}

    nothing = jnp.zeros((8, LANES), jnp.float32)

    def sum_rows(t, first, rows, carry):
        cols = pl.ds(t * LANES, LANES)

        def body(i, carry):
            acc, top = carry
            at = pl.ds(pl.multiple_of(first + i * 64, 64), 64)
            r = mix(sq_v[at, cols], wq_v[at, cols])
            res_q[at, cols] = r
            size = jnp.abs(r).reshape(8, 8, LANES)
            acc = acc + jnp.sum(size, axis=0)
            return acc, jnp.maximum(top, jnp.max(size, axis=0)) if t == 0 else top

        return lax.fori_loop(0, rows // 64, body, carry)

    def sum_tile(t):
        wait_bytes(wq_v.at[:, pl.ds(0, 2 * LANES)], in_sem.at[t])
        acc, _ = sum_rows(t, 0, ROWS, (nothing, nothing))
        sums[me, t] = jnp.sum(acc, axis=0, keepdims=True)

    def sum_first(part, acc):
        row, rows = (0, FIRST) if part == 0 else (FIRST, HALF - FIRST)
        wait_bytes(wq_v.at[pl.ds(0, rows), :], in_sem.at[part * TILES])
        carry = (acc, nothing)
        for half in range(2):
            carry = sum_rows(0, half * HALF + row, rows, carry)
        acc, top = carry
        top = jnp.maximum(jnp.max(top, axis=0, keepdims=True), 1e-30)
        sums[me, MAX_ROW + part] = top
        return acc, CODE / top

    def send_sums():
        for d in (4, 5, 3, 2, 6, 7, 1):
            pltpu.make_async_remote_copy(
                src_ref=sums.at[me],
                dst_ref=sums.at[me],
                send_sem=sum_send,
                recv_sem=sum_recv,
                device_id=group_peer(d),
                device_id_type=MESH,
            ).start()

    def final_place(origin, k):
        tile, row, rows, _ = UNITS[k]
        if tile < TILES:
            return out_q.at[pl.ds(pl.multiple_of((origin * 2 + c) * ROWS + row, 64), rows), pl.ds(tile * LANES, LANES)]
        return out_kv.at[:, pl.ds(pl.multiple_of((origin * 2 + c) * ROWS + row, HALF), rows)]

    def place(origin, k):
        _, row, rows, _ = UNITS[k]
        return coded.at[origin, pl.ds(row, rows)] if k < len(CODED) else final_place(origin, k)

    def unit_copy(ref, recv_sem, device):
        return pltpu.make_async_remote_copy(
            src_ref=ref, dst_ref=ref, send_sem=send_sem, recv_sem=recv_sem, device_id=device, device_id_type=MESH
        )

    to_right, to_left = {"zero_0": right}, {"zero_0": left}

    def send_right(k):
        unit_copy(place(x, k), side_recv.at[0, k], to_right).start()

    def send_left(k):
        unit_copy(place(x, k), side_recv.at[1, k], to_left).start()

    def relay(origin, k):
        unit_copy(final_place(origin, k), rel_recv, partner).start()

    def encode_rows(k, scale):
        _, row, rows, _ = UNITS[k]

        def body(i, carry):
            at = pl.ds(pl.multiple_of(row + i * 64, 64), 64)
            coded[x, at, :] = encode(res_q[at, 0:LANES], scale)
            return carry

        lax.fori_loop(0, rows // 64, body, 0)

    def decode_rows(origin, k, scale):
        _, row, rows, _ = UNITS[k]
        own = sums[origin * 2 + c, MAX_ROW + (k % 3 > 0)] * scale

        def body(i, carry):
            at = pl.multiple_of(row + i * 64, 64)
            there = pl.ds(pl.multiple_of((origin * 2 + c) * ROWS + at, 64), 64)
            out_q[there, 0:LANES] = (decode(coded[origin, pl.ds(at, 64), :]) * own).astype(jnp.bfloat16)
            return carry

        lax.fori_loop(0, rows // 64, body, 0)

    lane_of = lax.broadcasted_iota(jnp.int32, (KV, LANES), 1)
    diagonal = lane_of == lax.broadcasted_iota(jnp.int32, (KV, LANES), 0)

    acc, scale = sum_first(0, nothing)
    encode_rows(0, scale)
    encode_rows(3, scale)
    wait_for_neighbours()
    send_right(0)
    send_left(3)
    acc, scale = sum_first(1, acc)
    encode_rows(1, scale)
    send_right(1)
    encode_rows(4, scale)
    send_left(4)
    sums[me, 0] = jnp.sum(acc, axis=0, keepdims=True)
    wait_bytes(wq_v.at[pl.ds(0, 4 * 32 * ROWS // COLS), :], in_sem.at[KV_ROW + 1])
    acc = jnp.zeros((KV, LANES), jnp.float32)
    for j in range(ROWS // LANES):
        cols = pl.ds(j * LANES, LANES)
        r = mix(skv_v[:, cols], wkv_v[:, cols])
        res_kv[:, cols] = r
        acc = acc + jnp.abs(r)
    row_sums = jnp.sum(acc, axis=1, keepdims=True)
    sums[me, KV_ROW] = jnp.sum(jnp.where(diagonal, row_sums, 0.0), axis=0, keepdims=True)
    wait_bytes(norm_v, in_sem.at[NORM_ROW + 1])
    own_norm = norm_v[0] + norm_v[1]
    sums[me, NORM_ROW] = jnp.concatenate([own_norm, own_norm], axis=1)
    for t in range(1, TILES):
        sum_tile(t)
    wait_for_far()
    send_sums()
    encode_rows(2, scale)
    send_right(2)
    encode_rows(5, scale)
    for k in (5, 0, 1, 2):
        send_left(k)
    for k in (3, 4, 5):
        send_right(k)

    def factor_of(t):
        total = sums[0, t]
        for other in range(1, 8):
            total = total + sums[other, t]
        return total * (1.0 / D_MODEL)

    def narrow_tile(t):
        factor = factor_of(t)
        if t < TILES:
            fac_q[:, pl.ds(t * LANES, LANES)] = factor
            scale = 1.0 / factor
        else:
            fac_k[...] = factor[:, 0:32]
            fac_v[...] = pltpu.roll(factor, LANES - 32, 1)[:, 0:32]
            spread = jnp.sum(jnp.where(diagonal, jnp.broadcast_to(factor, (KV, LANES)), 0.0), axis=1, keepdims=True)
            scale = 1.0 / jnp.broadcast_to(spread, (KV, LANES))
        for half in range(2):
            if t < TILES:
                cols = pl.ds(t * LANES, LANES)

                def body(i, carry):
                    at = half * HALF + i * STEP
                    rows = pl.ds(pl.multiple_of(at, STEP), STEP)
                    there = pl.ds(pl.multiple_of(me * ROWS + at, STEP), STEP)
                    out_q[there, cols] = (res_q[rows, cols] * scale).astype(jnp.bfloat16)
                    return carry

                lax.fori_loop(0, HALF // STEP, body, 0)
            else:
                for j in range(HALF // LANES):
                    at = half * HALF + j * LANES
                    there = pl.ds(pl.multiple_of(me * ROWS + at, LANES), LANES)
                    out_kv[:, there] = (res_kv[:, pl.ds(at, LANES)] * scale).astype(jnp.bfloat16)
            k = len(CODED) + 2 * t - 2 + half
            for go_there in (send_right, send_left) if half == 0 else (send_left, send_right):
                go_there(k)
            relay(x, k)

    wait_bytes(sums.at[pl.ds(0, 7)], sum_recv)
    for t in range(1, TILES + 1):
        narrow_tile(t)
    first_factor = factor_of(0)
    fac_q[:, 0:LANES] = first_factor
    first_scale = 1.0 / (CODE * first_factor)
    for k in range(len(CODED)):
        decode_rows(x, k, first_scale)
        relay(x, k)

    def norm_copy(buf, at, stage, device):
        return pltpu.make_async_remote_copy(
            src_ref=buf.at[at],
            dst_ref=buf.at[at],
            send_sem=norm_send.at[stage],
            recv_sem=norm_recv.at[stage],
            device_id=device,
            device_id_type=MESH,
        )

    def norm_along_y():
        pl.semaphore_wait(barrier, 6)
        for other in range(8):
            norm_y[y, pl.ds(other, 1), :] = sums[other, NORM_ROW]
        for d in (2, 1, 3):
            norm_copy(norm_y, y, 0, {"width_1": lax.rem(y + d, 4)}).start()

    def norm_along_z():
        wait_bytes(norm_y.at[pl.ds(0, 3)], norm_recv.at[0])
        low = lax.broadcasted_iota(jnp.int32, (8, LANES), 1) < 64
        norm_z[z, 0] = jnp.where(low, norm_y[0], norm_y[1])
        norm_z[z, 1] = jnp.where(low, norm_y[2], norm_y[3])
        for d in (2, 1, 3):
            norm_copy(norm_z, z, 1, {"width_0": lax.rem(z + d, 4)}).start()

    def norm_end():
        wait_bytes(norm_z.at[pl.ds(0, 3)], norm_recv.at[1])
        for zz in range(4):
            for pair in range(2):
                for other in range(8):
                    norm_all[pl.ds(other * 8 + zz * 2 + pair, 1), :] = norm_z[zz, pair, pl.ds(other, 1), :]
        norm_out[...] = norm_all[...].astype(jnp.bfloat16)
        wait_bytes(norm_y.at[pl.ds(0, 3)], norm_send.at[0])
        wait_bytes(norm_z.at[pl.ds(0, 3)], norm_send.at[1])

    def norm_to_partner():
        return norm_copy(norm_out, pl.ds(0, 64), 2, partner)

    far = lax.rem(x + 2, 4)
    norm_steps = {2: norm_along_y, 4: norm_along_z, 6: norm_end, 7: lambda: norm_to_partner().start()}

    def hand_on(origin, k):
        if k < len(CODED):
            decode_rows(origin, k, first_scale)
        relay(origin, k)

    for i in range(len(UNITS)):
        for side in range(2):
            k, origin = ORDER[side][i], left if side == 0 else right
            unit_copy(place(origin, k), side_recv.at[side, k], partner).wait_recv()
            if UNITS[k][3] == side:
                unit_copy(place(origin, k), far_recv.at[k], to_right if side == 0 else to_left).start()
            hand_on(origin, k)
        if i in norm_steps:
            pl.when(c == 0)(norm_steps[i])
    pl.when(c == 0)(lambda: norm_to_partner().wait_send())
    pl.when(c == 1)(lambda: norm_to_partner().wait_recv())
    for k in (0, 3, 1, 4, 2, 5, *range(len(CODED), len(UNITS))):
        unit_copy(place(far, k), far_recv.at[k], partner).wait_recv()
        hand_on(far, k)

    shard_rows = ROWS + KV * ROWS // COLS
    wait_bytes(sums.at[pl.ds(0, 7)], sum_send)
    wait_bytes(out_q.at[pl.ds(0, 7 * shard_rows), :], send_sem)
    wait_bytes(out_q.at[pl.ds(0, 4 * shard_rows), :], rel_recv)


def write_kernel(
    out_q, out_kv, res_q, res_kv, fac_q, fac_k, fac_v, norm,
    final_q, final_k, final_v, factor_q, factor_k, factor_v, serve_norm, result_q, result_k, result_v, sem,
):
    def write(src, dst, which):
        pltpu.make_async_copy(src, dst, sem.at[which]).start()

    small = ((fac_q, factor_q), (fac_k, factor_k), (fac_v, factor_v), (norm, serve_norm))
    for i, (src, dst) in enumerate(small):
        write(src, dst, i)
    for part in range(8):
        rows = pl.ds(part * ROWS, ROWS)
        write(out_q.at[rows, :], final_q.at[rows, :], 4)
    write(res_q, result_q, 5)
    write(out_kv.at[pl.ds(0, 32), :], final_k, 6)
    write(out_kv.at[pl.ds(32, 32), :], final_v, 6)
    write(res_kv.at[pl.ds(0, 32), :], result_k, 7)
    write(res_kv.at[pl.ds(32, 32), :], result_v, 7)
    for i, ref in enumerate((fac_q, fac_k, fac_v, norm, out_q, res_q, out_kv, res_kv)):
        pltpu.make_async_copy(ref, ref, sem.at[i]).wait()


def on_device(weight_query, smooth_query, weight_key, smooth_key, weight_value, smooth_value, norm_train, norm_step):
    f32, bf16 = jnp.float32, jnp.bfloat16
    any_spec, vmem_spec = pl.BlockSpec(memory_space=pl.ANY), pl.BlockSpec(memory_space=pltpu.VMEM)
    held = (
        ((D_MODEL, COLS), bf16),
        ((KV, D_MODEL), bf16),
        ((ROWS, COLS), f32),
        ((KV, ROWS), f32),
        ((1, COLS), f32),
        ((1, 32), f32),
        ((1, 32), f32),
        ((64, LANES), bf16),
    )
    units = len(UNITS)
    dma = pltpu.SemaphoreType.DMA
    gathered = pl.pallas_call(
        gather_kernel,
        out_shape=tuple(pltpu.VMEM(shape, dtype) for shape, dtype in held),
        in_specs=[any_spec] * 8,
        out_specs=tuple(vmem_spec for _ in held),
        scratch_shapes=[
            pltpu.VMEM((ROWS, COLS), f32),
            pltpu.VMEM((ROWS, COLS), f32),
            pltpu.VMEM((KV, ROWS), f32),
            pltpu.VMEM((KV, ROWS), f32),
            pltpu.VMEM((2, 1, 64), f32),
            pltpu.VMEM((4, ROWS, LANES), bf16),
            pltpu.VMEM((8, SUM_ROWS, 1, LANES), f32),
            pltpu.VMEM((4, 8, LANES), f32),
            pltpu.VMEM((4, 2, 8, LANES), f32),
            pltpu.VMEM((64, LANES), f32),
            dma((NORM_ROW + 2,)),
            dma,
            dma,
            dma,
            dma((2, units)),
            dma((units,)),
            dma,
            dma((3,)),
            dma((3,)),
            pltpu.SemaphoreType.REGULAR((2,)),
            pltpu.SemaphoreType.REGULAR,
        ],
        compiler_params=pltpu.CompilerParams(
            collective_id=0, has_side_effects=True, vmem_limit_bytes=16 * 1024 * 1024
        ),
        name="gather",
    )(
        *(
            pltpu.with_memory_space_constraint(a, pltpu.HBM)
            for a in (
                weight_query, smooth_query, weight_key.T, smooth_key.T, weight_value.T, smooth_value.T,
                norm_train.reshape(1, 64), norm_step.reshape(1, 64),
            )
        )
    )
    outs = (
        ((D_MODEL, COLS), bf16),
        ((32, D_MODEL), bf16),
        ((32, D_MODEL), bf16),
        ((1, COLS), f32),
        ((1, 32), f32),
        ((1, 32), f32),
        ((64, LANES), bf16),
        ((ROWS, COLS), f32),
        ((32, ROWS), f32),
        ((32, ROWS), f32),
    )
    fq, fk, fv, cq, ck, cv, norm, rq, rk, rv = pl.pallas_call(
        write_kernel,
        out_shape=tuple(jax.ShapeDtypeStruct(shape, dtype) for shape, dtype in outs),
        in_specs=[vmem_spec] * len(held),
        out_specs=tuple(any_spec for _ in outs),
        scratch_shapes=[dma((8,))],
        compiler_params=pltpu.CompilerParams(vmem_limit_bytes=4 * 1024 * 1024),
        name="write",
    )(*gathered)
    return (
        fq, fk.T, fv.T, cq.reshape(COLS), ck.reshape(32), cv.reshape(32), norm.reshape(D_MODEL), rq, rk.T, rv.T
    )


def solution(mesh):
    split = Mesh(mesh.devices.reshape(4, 2, 4, 4), ("zero_0", "zero_1", "width_0", "width_1"))
    in_specs = (
        P(ZERO, WIDTH),
        P(ZERO, WIDTH),
        P(ZERO, WIDTH),
        P(ZERO, WIDTH),
        P(ZERO, WIDTH),
        P(ZERO, WIDTH),
        P(ZERO_WIDTH),
        P(ZERO_WIDTH),
    )
    out_specs = (
        P(None, WIDTH),
        P(None, WIDTH),
        P(None, WIDTH),
        P(WIDTH),
        P(WIDTH),
        P(WIDTH),
        P(),
        P(ZERO, WIDTH),
        P(ZERO, WIDTH),
        P(ZERO, WIDTH),
    )
    return jax.shard_map(
        on_device, mesh=split, in_specs=in_specs, out_specs=out_specs, check_vma=False
    )
```

```python
import jax
import jax.numpy as jnp
from jax import lax
from jax.experimental import pallas as pl
from jax.experimental.pallas import tpu as pltpu
from jax.sharding import Mesh
from jax.sharding import PartitionSpec as P

D_MODEL = 8192
ZERO = ("zero_0", "zero_1")
ZERO_WIDTH = ("zero_0", "zero_1", "width_0", "width_1")
WIDTH = ("width_0", "width_1")
MESH = pl.DeviceIdType.MESH

keep_rate = 0.7

ROWS = 1024
COLS = 512
HALF = ROWS // 2
KV = 64
LANES = 128
TILES = COLS // LANES
STEP = 128
KV_ROW, NORM_ROW, MAX_ROW = TILES, TILES + 1, TILES + 2
SUM_ROWS = TILES + 4

FIRST = 192
PIECES = ((0, FIRST), (192, 128), (320, 192))
CODED = tuple((0, half * HALF + row, rows, half) for half in range(2) for row, rows in PIECES)
UNITS = CODED + tuple((tile, half * HALF, HALF, half) for tile in range(1, TILES + 1) for half in range(2))
KV_UNITS = (len(UNITS) - 2, len(UNITS) - 1)
SIDE_GROUPS = ((0, 1, 2), (3, 4, 5), *((k, k + 1) for k in range(6, len(UNITS), 2)))
FAR_GROUPS = ((0, 1, 2), (3, 4, 5), (6, 8), (7, 9), (10,), (11,), (12,), (13,))
SIDE_OF = {k: g for g, units in enumerate(SIDE_GROUPS) for k in units}
FAR_OF = {k: g for g, units in enumerate(FAR_GROUPS) for k in units}
CODE = 180.0


def mix(smooth, weight):
    return keep_rate * smooth + (1.0 - keep_rate) * weight


def encode(x, scale):
    v = x * scale
    for _ in range(4):
        v = v * v
    return jnp.where(x < 0, -v, v).astype(jnp.bfloat16)


def decode(code):
    v = code.astype(jnp.float32)
    root = jnp.abs(v)
    for _ in range(4):
        root = lax.rsqrt(root)
    return jnp.where(v < 0, -root, root)


def gather_kernel(
    wq, sq, wk, sk, wv, sv, norm_a, norm_b,
    out_q, out_kv, res_q, res_kv, fac_q, fac_k, fac_v, norm_out,
    wq_v, sq_v, wkv_v, skv_v, norm_v, coded, sums, norm_y, norm_z, norm_all,
    in_sem, send_sem, extra_send, sum_send, sum_recv, side_recv, far_recv, rel_recv, kv_recv, far_kv_recv,
    norm_send, norm_recv, go, vouch,
):
    x, c = lax.axis_index("zero_0"), lax.axis_index("zero_1")
    z, y = lax.axis_index("width_0"), lax.axis_index("width_1")
    me = x * 2 + c
    right, left = lax.rem(x + 1, 4), lax.rem(x + 3, 4)
    partner = {"zero_1": 1 - c}

    def load(src, dst, which):
        pltpu.make_async_copy(src, dst, in_sem.at[which]).start()

    def load_rows(t, first, rows, which):
        at = (pl.ds(first, rows), pl.ds(t * LANES, LANES))
        load(wq.at[at], wq_v.at[at], which)
        load(sq.at[at], sq_v.at[at], which)

    def wait_bytes(ref, sem):
        pltpu.make_async_copy(ref, ref, sem).wait()

    barrier = pltpu.get_barrier_semaphore()
    for device in ({"zero_0": right, "zero_1": 1}, {"zero_0": left, "zero_1": 1}):
        pl.semaphore_signal(barrier, inc=1, device_id=device, device_id_type=MESH)

    @pl.when(c == 0)
    def _():
        pl.semaphore_signal(barrier, inc=1, device_id=partner, device_id_type=MESH)

    for row in (0, HALF):
        load_rows(0, row, FIRST, 0)
    for row in (FIRST, HALF + FIRST):
        load_rows(0, row, HALF - FIRST, TILES)
    load(wk, wkv_v.at[pl.ds(0, 32), :], KV_ROW + 1)
    load(sk, skv_v.at[pl.ds(0, 32), :], KV_ROW + 1)
    load(wv, wkv_v.at[pl.ds(32, 32), :], KV_ROW + 1)
    load(sv, skv_v.at[pl.ds(32, 32), :], KV_ROW + 1)
    load(norm_a, norm_v.at[0], NORM_ROW + 1)
    load(norm_b, norm_v.at[1], NORM_ROW + 1)
    for t in range(1, TILES):
        load_rows(t, 0, ROWS, t)

    @pl.when(c == 0)
    def _():
        for d in (2, 1, 3):
            pl.semaphore_signal(barrier, inc=1, device_id={"width_1": lax.rem(y + d, 4)}, device_id_type=MESH)
            pl.semaphore_signal(barrier, inc=1, device_id={"width_0": lax.rem(z + d, 4)}, device_id_type=MESH)

    def wait_for_neighbours():
        @pl.when(c == 1)
        def _():
            pl.semaphore_wait(barrier, 5)
            pl.semaphore_signal(go.at[0], inc=1, device_id=partner, device_id_type=MESH)
            for side in (left, right):
                pl.semaphore_signal(vouch, inc=1, device_id={"zero_0": side}, device_id_type=MESH)

        @pl.when(c == 0)
        def _():
            pl.semaphore_wait(go.at[0], 1)

    def wait_for_far():
        @pl.when(c == 1)
        def _():
            pl.semaphore_wait(vouch, 2)
            pl.semaphore_signal(go.at[1], inc=1, device_id=partner, device_id_type=MESH)

        @pl.when(c == 0)
        def _():
            pl.semaphore_wait(go.at[1], 1)

    def group_peer(d):
        other = lax.rem(me + d, 8)
        return {"zero_0": other // 2, "zero_1": lax.rem(other, 2)}

    nothing = jnp.zeros((8, LANES), jnp.float32)

    def sum_rows(t, first, rows, carry):
        cols = pl.ds(t * LANES, LANES)

        def body(i, carry):
            acc, top = carry
            at = pl.ds(pl.multiple_of(first + i * 64, 64), 64)
            r = mix(sq_v[at, cols], wq_v[at, cols])
            res_q[at, cols] = r
            size = jnp.abs(r).reshape(8, 8, LANES)
            acc = acc + jnp.sum(size, axis=0)
            return acc, jnp.maximum(top, jnp.max(size, axis=0)) if t == 0 else top

        return lax.fori_loop(0, rows // 64, body, carry)

    def sum_tile(t):
        wait_bytes(wq_v.at[:, pl.ds(0, 2 * LANES)], in_sem.at[t])
        acc, _ = sum_rows(t, 0, ROWS, (nothing, nothing))
        sums[me, t] = jnp.sum(acc, axis=0, keepdims=True)

    def sum_first(part, acc):
        row, rows = (0, FIRST) if part == 0 else (FIRST, HALF - FIRST)
        wait_bytes(wq_v.at[pl.ds(0, rows), :], in_sem.at[part * TILES])
        carry = (acc, nothing)
        for half in range(2):
            carry = sum_rows(0, half * HALF + row, rows, carry)
        acc, top = carry
        top = jnp.maximum(jnp.max(top, axis=0, keepdims=True), 1e-30)
        sums[me, MAX_ROW + part] = top
        return acc, CODE / top

    def send_sums():
        for d in (4, 5, 3, 2, 6, 7, 1):
            pltpu.make_async_remote_copy(
                src_ref=sums.at[me],
                dst_ref=sums.at[me],
                send_sem=sum_send,
                recv_sem=sum_recv,
                device_id=group_peer(d),
                device_id_type=MESH,
            ).start()

    def final_place(origin, k, core):
        tile, row, rows, _ = UNITS[k]
        at = (origin * 2 + core) * ROWS + row
        if tile < TILES:
            return out_q.at[pl.ds(pl.multiple_of(at, 64), rows), pl.ds(tile * LANES, LANES)]
        return out_kv.at[:, pl.ds(pl.multiple_of(at, HALF), rows)]

    def place(origin, k):
        _, row, rows, _ = UNITS[k]
        return coded.at[origin, pl.ds(row, rows)] if k < len(CODED) else final_place(origin, k, c)

    def unit_copy(ref, recv_sem, device, sem=send_sem):
        return pltpu.make_async_remote_copy(
            src_ref=ref, dst_ref=ref, send_sem=sem, recv_sem=recv_sem, device_id=device, device_id_type=MESH
        )

    def wait_units(units, sem):
        rows = sum(64 * HALF // LANES if k >= KV_UNITS[0] else UNITS[k][2] for k in units)
        wait_bytes(out_q.at[pl.ds(0, rows), pl.ds(0, LANES)], sem)

    to_right, to_left = {"zero_0": right}, {"zero_0": left}

    def send_right(k):
        unit_copy(place(x, k), side_recv.at[0, SIDE_OF[k]], to_right).start()

    def send_left(k):
        unit_copy(place(x, k), side_recv.at[1, SIDE_OF[k]], to_left).start()

    def relay(origin, k):
        unit_copy(final_place(origin, k, c), rel_recv, partner).start()

    def encode_rows(k, scale):
        _, row, rows, _ = UNITS[k]

        def body(i, carry):
            at = pl.ds(pl.multiple_of(row + i * 64, 64), 64)
            coded[x, at, :] = encode(res_q[at, 0:LANES], scale)
            return carry

        lax.fori_loop(0, rows // 64, body, 0)

    def decode_rows(origin, k, scale):
        _, row, rows, _ = UNITS[k]
        own = sums[origin * 2 + c, MAX_ROW + (k % 3 > 0)] * scale

        def body(i, carry):
            at = pl.multiple_of(row + i * 64, 64)
            there = pl.ds(pl.multiple_of((origin * 2 + c) * ROWS + at, 64), 64)
            out_q[there, 0:LANES] = (decode(coded[origin, pl.ds(at, 64), :]) * own).astype(jnp.bfloat16)
            return carry

        lax.fori_loop(0, rows // 64, body, 0)

    lane_of = lax.broadcasted_iota(jnp.int32, (KV, LANES), 1)
    diagonal = lane_of == lax.broadcasted_iota(jnp.int32, (KV, LANES), 0)

    acc, scale = sum_first(0, nothing)
    encode_rows(0, scale)
    encode_rows(3, scale)
    wait_for_neighbours()
    send_right(0)
    send_left(3)
    acc, scale = sum_first(1, acc)
    encode_rows(1, scale)
    send_right(1)
    encode_rows(4, scale)
    send_left(4)
    sums[me, 0] = jnp.sum(acc, axis=0, keepdims=True)
    wait_bytes(wq_v.at[pl.ds(0, 4 * 32 * ROWS // COLS), :], in_sem.at[KV_ROW + 1])
    acc = jnp.zeros((KV, LANES), jnp.float32)
    for j in range(ROWS // LANES):
        cols = pl.ds(j * LANES, LANES)
        r = mix(skv_v[:, cols], wkv_v[:, cols])
        res_kv[:, cols] = r
        acc = acc + jnp.abs(r)
    row_sums = jnp.sum(acc, axis=1, keepdims=True)
    sums[me, KV_ROW] = jnp.sum(jnp.where(diagonal, row_sums, 0.0), axis=0, keepdims=True)
    wait_bytes(norm_v, in_sem.at[NORM_ROW + 1])
    own_norm = norm_v[0] + norm_v[1]
    sums[me, NORM_ROW] = jnp.concatenate([own_norm, own_norm], axis=1)
    for t in range(1, TILES):
        sum_tile(t)
    wait_for_far()
    send_sums()
    encode_rows(2, scale)
    send_right(2)
    encode_rows(5, scale)
    for k in (5, 0, 1, 2):
        send_left(k)
    for k in (3, 4, 5):
        send_right(k)

    def factor_of(t):
        total = sums[0, t]
        for other in range(1, 8):
            total = total + sums[other, t]
        return total * (1.0 / D_MODEL)

    def narrow_tile(t):
        factor = factor_of(t)
        if t < TILES:
            fac_q[:, pl.ds(t * LANES, LANES)] = factor
            scale = 1.0 / factor
        else:
            fac_k[...] = factor[:, 0:32]
            fac_v[...] = pltpu.roll(factor, LANES - 32, 1)[:, 0:32]
            spread = jnp.sum(jnp.where(diagonal, jnp.broadcast_to(factor, (KV, LANES)), 0.0), axis=1, keepdims=True)
            scale = 1.0 / jnp.broadcast_to(spread, (KV, LANES))
        for half in range(2):
            if t < TILES:
                cols = pl.ds(t * LANES, LANES)

                def body(i, carry):
                    at = half * HALF + i * STEP
                    rows = pl.ds(pl.multiple_of(at, STEP), STEP)
                    there = pl.ds(pl.multiple_of(me * ROWS + at, STEP), STEP)
                    out_q[there, cols] = (res_q[rows, cols] * scale).astype(jnp.bfloat16)
                    return carry

                lax.fori_loop(0, HALF // STEP, body, 0)
            else:
                for j in range(HALF // LANES):
                    at = half * HALF + j * LANES
                    there = pl.ds(pl.multiple_of(me * ROWS + at, LANES), LANES)
                    out_kv[:, there] = (res_kv[:, pl.ds(at, LANES)] * scale).astype(jnp.bfloat16)
            k = len(CODED) + 2 * t - 2 + half
            for go_there in (send_right, send_left) if half == 0 else (send_left, send_right):
                go_there(k)
            relay(x, k)

    wait_bytes(sums.at[pl.ds(0, 7)], sum_recv)
    for t in range(1, TILES + 1):
        narrow_tile(t)
    first_factor = factor_of(0)
    fac_q[:, 0:LANES] = first_factor
    first_scale = 1.0 / (CODE * first_factor)
    for k in range(len(CODED)):
        decode_rows(x, k, first_scale)
        relay(x, k)

    def norm_copy(buf, at, stage, device):
        return pltpu.make_async_remote_copy(
            src_ref=buf.at[at],
            dst_ref=buf.at[at],
            send_sem=norm_send.at[stage],
            recv_sem=norm_recv.at[stage],
            device_id=device,
            device_id_type=MESH,
        )

    def norm_along_y():
        pl.semaphore_wait(barrier, 6)
        for other in range(8):
            norm_y[y, pl.ds(other, 1), :] = sums[other, NORM_ROW]
        for d in (2, 1, 3):
            norm_copy(norm_y, y, 0, {"width_1": lax.rem(y + d, 4)}).start()

    def norm_along_z():
        wait_bytes(norm_y.at[pl.ds(0, 3)], norm_recv.at[0])
        low = lax.broadcasted_iota(jnp.int32, (8, LANES), 1) < 64
        norm_z[z, 0] = jnp.where(low, norm_y[0], norm_y[1])
        norm_z[z, 1] = jnp.where(low, norm_y[2], norm_y[3])
        for d in (2, 1, 3):
            norm_copy(norm_z, z, 1, {"width_0": lax.rem(z + d, 4)}).start()

    def norm_end():
        wait_bytes(norm_z.at[pl.ds(0, 3)], norm_recv.at[1])
        for zz in range(4):
            for pair in range(2):
                for other in range(8):
                    norm_all[pl.ds(other * 8 + zz * 2 + pair, 1), :] = norm_z[zz, pair, pl.ds(other, 1), :]
        norm_out[...] = norm_all[...].astype(jnp.bfloat16)
        wait_bytes(norm_y.at[pl.ds(0, 3)], norm_send.at[0])
        wait_bytes(norm_z.at[pl.ds(0, 3)], norm_send.at[1])

    def norm_to_partner():
        return norm_copy(norm_out, pl.ds(0, 64), 2, partner)

    far = lax.rem(x + 2, 4)
    norm_steps = {1: norm_along_y, 2: norm_along_z, 3: norm_end, 4: lambda: norm_to_partner().start()}

    def hand_on(origin, k):
        if k < len(CODED):
            decode_rows(origin, k, first_scale)
        relay(origin, k)

    def forward(origin, k):
        unit_copy(place(origin, k), far_recv.at[FAR_OF[k]], to_left if UNITS[k][3] else to_right).start()

    for i in range(len(SIDE_GROUPS)):
        for side in range(2):
            group = i if i > 1 or side == 0 else 1 - i
            units, origin = SIDE_GROUPS[group], left if side == 0 else right
            wait_units(units, side_recv.at[side, group])
            for k in units:
                if UNITS[k][3] == side and k in KV_UNITS:

                    @pl.when(c == 1)
                    def _():
                        forward(origin, k)
                        relay(origin, k)

                    @pl.when(c == 0)
                    def _():
                        unit_copy(final_place(origin, k, 0), kv_recv.at[side], partner).start()
                    continue
                if UNITS[k][3] == side:
                    forward(origin, k)
                hand_on(origin, k)
        if i in norm_steps:
            pl.when(c == 0)(norm_steps[i])

    @pl.when(c == 1)
    def _():
        for side, origin, device in ((0, left, to_right), (1, right, to_left)):
            k = KV_UNITS[side]
            wait_units((k,), kv_recv.at[side])
            unit_copy(final_place(origin, k, 0), far_kv_recv.at[side], device, extra_send).start()

    pl.when(c == 0)(lambda: norm_to_partner().wait_send())
    pl.when(c == 1)(lambda: norm_to_partner().wait_recv())
    for group, units in enumerate(FAR_GROUPS):
        if units[0] in KV_UNITS:
            continue
        wait_units(units, far_recv.at[group])
        for k in units:
            hand_on(far, k)

    @pl.when(c == 1)
    def _():
        for k in KV_UNITS:
            wait_units((k,), far_recv.at[FAR_OF[k]])
            relay(far, k)
        for side, k in enumerate(KV_UNITS):
            wait_units((k,), far_kv_recv.at[side])
            unit_copy(final_place(far, k, 0), rel_recv, partner, extra_send).start()

    share = ROWS + KV * ROWS // COLS
    kv_rows = KV * ROWS // COLS

    wait_bytes(sums.at[pl.ds(0, 7)], sum_send)

    @pl.when(c == 1)
    def _():
        wait_bytes(out_q.at[pl.ds(0, 7 * share), :], send_sem)
        wait_bytes(out_q.at[pl.ds(0, 2 * kv_rows), :], extra_send)
        wait_bytes(out_q.at[pl.ds(0, 4 * share - 2 * kv_rows), :], rel_recv)

    @pl.when(c == 0)
    def _():
        wait_bytes(out_q.at[pl.ds(0, 7 * share - 2 * kv_rows), :], send_sem)
        wait_bytes(out_q.at[pl.ds(0, 4 * share + kv_rows), :], rel_recv)


def write_kernel(
    out_q, out_kv, res_q, res_kv, fac_q, fac_k, fac_v, norm,
    final_q, final_k, final_v, factor_q, factor_k, factor_v, serve_norm, result_q, result_k, result_v, sem,
):
    def write(src, dst, which):
        pltpu.make_async_copy(src, dst, sem.at[which]).start()

    small = ((fac_q, factor_q), (fac_k, factor_k), (fac_v, factor_v), (norm, serve_norm))
    for i, (src, dst) in enumerate(small):
        write(src, dst, i)
    for part in range(8):
        rows = pl.ds(part * ROWS, ROWS)
        write(out_q.at[rows, :], final_q.at[rows, :], 4)
    write(res_q, result_q, 5)
    write(out_kv.at[pl.ds(0, 32), :], final_k, 6)
    write(out_kv.at[pl.ds(32, 32), :], final_v, 6)
    write(res_kv.at[pl.ds(0, 32), :], result_k, 7)
    write(res_kv.at[pl.ds(32, 32), :], result_v, 7)
    for i, ref in enumerate((fac_q, fac_k, fac_v, norm, out_q, res_q, out_kv, res_kv)):
        pltpu.make_async_copy(ref, ref, sem.at[i]).wait()


def on_device(weight_query, smooth_query, weight_key, smooth_key, weight_value, smooth_value, norm_train, norm_step):
    f32, bf16 = jnp.float32, jnp.bfloat16
    any_spec, vmem_spec = pl.BlockSpec(memory_space=pl.ANY), pl.BlockSpec(memory_space=pltpu.VMEM)
    held = (
        ((D_MODEL, COLS), bf16),
        ((KV, D_MODEL), bf16),
        ((ROWS, COLS), f32),
        ((KV, ROWS), f32),
        ((1, COLS), f32),
        ((1, 32), f32),
        ((1, 32), f32),
        ((64, LANES), bf16),
    )
    dma = pltpu.SemaphoreType.DMA
    gathered = pl.pallas_call(
        gather_kernel,
        out_shape=tuple(pltpu.VMEM(shape, dtype) for shape, dtype in held),
        in_specs=[any_spec] * 8,
        out_specs=tuple(vmem_spec for _ in held),
        scratch_shapes=[
            pltpu.VMEM((ROWS, COLS), f32),
            pltpu.VMEM((ROWS, COLS), f32),
            pltpu.VMEM((KV, ROWS), f32),
            pltpu.VMEM((KV, ROWS), f32),
            pltpu.VMEM((2, 1, 64), f32),
            pltpu.VMEM((4, ROWS, LANES), bf16),
            pltpu.VMEM((8, SUM_ROWS, 1, LANES), f32),
            pltpu.VMEM((4, 8, LANES), f32),
            pltpu.VMEM((4, 2, 8, LANES), f32),
            pltpu.VMEM((64, LANES), f32),
            dma((NORM_ROW + 2,)),
            dma,
            dma,
            dma,
            dma,
            dma((2, len(SIDE_GROUPS))),
            dma((len(FAR_GROUPS),)),
            dma,
            dma((2,)),
            dma((2,)),
            dma((3,)),
            dma((3,)),
            pltpu.SemaphoreType.REGULAR((2,)),
            pltpu.SemaphoreType.REGULAR,
        ],
        compiler_params=pltpu.CompilerParams(
            collective_id=0, has_side_effects=True, vmem_limit_bytes=16 * 1024 * 1024
        ),
        name="gather",
    )(
        *(
            pltpu.with_memory_space_constraint(a, pltpu.HBM)
            for a in (
                weight_query, smooth_query, weight_key.T, smooth_key.T, weight_value.T, smooth_value.T,
                norm_train.reshape(1, 64), norm_step.reshape(1, 64),
            )
        )
    )
    outs = (
        ((D_MODEL, COLS), bf16),
        ((32, D_MODEL), bf16),
        ((32, D_MODEL), bf16),
        ((1, COLS), f32),
        ((1, 32), f32),
        ((1, 32), f32),
        ((64, LANES), bf16),
        ((ROWS, COLS), f32),
        ((32, ROWS), f32),
        ((32, ROWS), f32),
    )
    fq, fk, fv, cq, ck, cv, norm, rq, rk, rv = pl.pallas_call(
        write_kernel,
        out_shape=tuple(jax.ShapeDtypeStruct(shape, dtype) for shape, dtype in outs),
        in_specs=[vmem_spec] * len(held),
        out_specs=tuple(any_spec for _ in outs),
        scratch_shapes=[dma((8,))],
        compiler_params=pltpu.CompilerParams(vmem_limit_bytes=4 * 1024 * 1024),
        name="write",
    )(*gathered)
    return (
        fq, fk.T, fv.T, cq.reshape(COLS), ck.reshape(32), cv.reshape(32), norm.reshape(D_MODEL), rq, rk.T, rv.T
    )


def solution(mesh):
    split = Mesh(mesh.devices.reshape(4, 2, 4, 4), ("zero_0", "zero_1", "width_0", "width_1"))
    in_specs = (
        P(ZERO, WIDTH),
        P(ZERO, WIDTH),
        P(ZERO, WIDTH),
        P(ZERO, WIDTH),
        P(ZERO, WIDTH),
        P(ZERO, WIDTH),
        P(ZERO_WIDTH),
        P(ZERO_WIDTH),
    )
    out_specs = (
        P(None, WIDTH),
        P(None, WIDTH),
        P(None, WIDTH),
        P(WIDTH),
        P(WIDTH),
        P(WIDTH),
        P(),
        P(ZERO, WIDTH),
        P(ZERO, WIDTH),
        P(ZERO, WIDTH),
    )
    return jax.shard_map(
        on_device, mesh=split, in_specs=in_specs, out_specs=out_specs, check_vma=False
    )
```

```python
import jax
import jax.numpy as jnp
from jax import lax
from jax.experimental import pallas as pl
from jax.experimental.pallas import tpu as pltpu
from jax.sharding import Mesh
from jax.sharding import PartitionSpec as P

D_MODEL = 8192
ZERO = ("zero_0", "zero_1")
ZERO_WIDTH = ("zero_0", "zero_1", "width_0", "width_1")
WIDTH = ("width_0", "width_1")
MESH = pl.DeviceIdType.MESH

keep_rate = 0.7

ROWS = 1024
COLS = 512
HALF = ROWS // 2
KV = 64
LANES = 128
TILES = COLS // LANES
STEP = 128
STEPS = {96: 96, 288: 96, 128: 128, 416: 104, ROWS: STEP}
KV_ROW, NORM_ROW, MAX_ROW = TILES, TILES + 1, TILES + 2
ROW_OF = (1, 0, 2, 3, KV_ROW)
SUM_ROWS = TILES + 4

FIRST = 96
PIECES = ((0, FIRST), (FIRST, 288), (384, 128))
CODED = tuple((0, half * HALF + row, rows, half) for half in range(2) for row, rows in PIECES)
QUARTER = HALF // 2
UNITS = (
    *CODED,
    *((tile, half * HALF, HALF, half) for tile in range(1, TILES - 1) for half in range(2)),
    *((TILES - 1, part * QUARTER, QUARTER, part // 2) for part in range(4)),
    *((TILES, half * HALF, HALF, half) for half in range(2)),
)
FIRST_OF = tuple(min(k for k, unit in enumerate(UNITS) if unit[0] == tile) for tile in range(TILES + 1))
KV_UNITS = (len(UNITS) - 2, len(UNITS) - 1)
SIDE_GROUPS = ((0, 1, 2), (3, 4, 5), (6, 7, 8, 9), (10, 11, 12, 13, 14, 15))
FAR_GROUPS = ((0, 1, 2), (3, 4, 5), (6, 8), (7, 9), (10,), (12,), (11,), (13,), (14,), (15,))
SIDE_OF = {k: g for g, units in enumerate(SIDE_GROUPS) for k in units}
FAR_OF = {k: g for g, units in enumerate(FAR_GROUPS) for k in units}
CODE = 180.0


def mix(smooth, weight):
    return keep_rate * smooth + (1.0 - keep_rate) * weight


def encode(x, scale):
    v = x * scale
    for _ in range(4):
        v = v * v
    return jnp.where(x < 0, -v, v).astype(jnp.bfloat16)


def decode(code):
    v = code.astype(jnp.float32)
    root = jnp.abs(v)
    for _ in range(4):
        root = lax.rsqrt(root)
    return jnp.where(v < 0, -root, root)


def gather_kernel(
    wq, sq, wk, sk, wv, sv, norm_a, norm_b,
    out_q, out_kv, res_q, res_kv, fac_q, fac_k, fac_v, norm_out,
    wq_v, sq_v, wkv_v, skv_v, norm_v, coded, sums, norm_y, norm_z, norm_all,
    in_sem, send_sem, extra_send, sum_send, sum_recv, side_recv, far_recv, rel_recv, kv_recv, far_kv_recv,
    norm_send, norm_recv, go, vouch,
):
    x, c = lax.axis_index("zero_0"), lax.axis_index("zero_1")
    z, y = lax.axis_index("width_0"), lax.axis_index("width_1")
    me = x * 2 + c
    right, left = lax.rem(x + 1, 4), lax.rem(x + 3, 4)
    partner = {"zero_1": 1 - c}

    def load(src, dst, which):
        pltpu.make_async_copy(src, dst, in_sem.at[which]).start()

    def load_rows(t, first, rows, which):
        at = (pl.ds(first, rows), pl.ds(t * LANES, LANES))
        load(wq.at[at], wq_v.at[at], which)
        load(sq.at[at], sq_v.at[at], which)

    def wait_bytes(ref, sem):
        pltpu.make_async_copy(ref, ref, sem).wait()

    barrier = pltpu.get_barrier_semaphore()
    for device in ({"zero_0": right, "zero_1": 1}, {"zero_0": left, "zero_1": 1}):
        pl.semaphore_signal(barrier, inc=1, device_id=device, device_id_type=MESH)

    @pl.when(c == 0)
    def _():
        pl.semaphore_signal(barrier, inc=1, device_id=partner, device_id_type=MESH)

    for row in (0, HALF):
        load_rows(0, row, FIRST, 0)
    for row in (FIRST, HALF + FIRST):
        load_rows(0, row, HALF - FIRST, TILES)
    load_rows(1, 0, ROWS, 1)
    load(wk, wkv_v.at[pl.ds(0, 32), :], KV_ROW + 1)
    load(sk, skv_v.at[pl.ds(0, 32), :], KV_ROW + 1)
    load(wv, wkv_v.at[pl.ds(32, 32), :], KV_ROW + 1)
    load(sv, skv_v.at[pl.ds(32, 32), :], KV_ROW + 1)
    load(norm_a, norm_v.at[0], NORM_ROW + 1)
    load(norm_b, norm_v.at[1], NORM_ROW + 1)
    for t in range(2, TILES):
        load_rows(t, 0, ROWS, t)

    @pl.when(c == 0)
    def _():
        for d in (2, 1, 3):
            pl.semaphore_signal(barrier, inc=1, device_id={"width_1": lax.rem(y + d, 4)}, device_id_type=MESH)
            pl.semaphore_signal(barrier, inc=1, device_id={"width_0": lax.rem(z + d, 4)}, device_id_type=MESH)

    def wait_for_neighbours():
        @pl.when(c == 1)
        def _():
            pl.semaphore_wait(barrier, 5)
            pl.semaphore_signal(go.at[0], inc=1, device_id=partner, device_id_type=MESH)
            for side in (left, right):
                pl.semaphore_signal(vouch, inc=1, device_id={"zero_0": side}, device_id_type=MESH)

        @pl.when(c == 0)
        def _():
            pl.semaphore_wait(go.at[0], 1)

    def wait_for_far():
        @pl.when(c == 1)
        def _():
            pl.semaphore_wait(vouch, 2)
            pl.semaphore_signal(go.at[1], inc=1, device_id=partner, device_id_type=MESH)

        @pl.when(c == 0)
        def _():
            pl.semaphore_wait(go.at[1], 1)

    def group_peer(d):
        other = lax.rem(me + d, 8)
        return {"zero_0": other // 2, "zero_1": lax.rem(other, 2)}

    nothing = jnp.zeros((8, LANES), jnp.float32)

    def sum_rows(t, first, rows, carry):
        cols = pl.ds(t * LANES, LANES)
        step = STEPS[rows]

        def body(i, carry):
            acc, top = carry
            at = pl.ds(pl.multiple_of(first + i * step, 8), step)
            r = mix(sq_v[at, cols], wq_v[at, cols])
            res_q[at, cols] = r
            size = jnp.abs(r).reshape(step // 8, 8, LANES)
            acc = acc + jnp.sum(size, axis=0)
            return acc, jnp.maximum(top, jnp.max(size, axis=0)) if t == 0 else top

        return lax.fori_loop(0, rows // step, body, carry)

    def sum_tile(t):
        wait_bytes(wq_v.at[:, pl.ds(0, 2 * LANES)], in_sem.at[t])
        acc, _ = sum_rows(t, 0, ROWS, (nothing, nothing))
        sums[me, ROW_OF[t]] = jnp.sum(acc, axis=0, keepdims=True)

    def sum_first(part, acc):
        row, rows = (0, FIRST) if part == 0 else (FIRST, HALF - FIRST)
        wait_bytes(wq_v.at[pl.ds(0, rows), :], in_sem.at[part * TILES])
        carry = (acc, nothing)
        for half in range(2):
            carry = sum_rows(0, half * HALF + row, rows, carry)
        acc, top = carry
        top = jnp.maximum(jnp.max(top, axis=0, keepdims=True), 1e-30)
        sums[me, MAX_ROW + part] = top
        return acc, CODE / top

    def send_sums(first, count, which):
        for d in (4, 5, 3, 2, 6, 7, 1):
            pltpu.make_async_remote_copy(
                src_ref=sums.at[me, pl.ds(first, count)],
                dst_ref=sums.at[me, pl.ds(first, count)],
                send_sem=sum_send,
                recv_sem=sum_recv.at[which],
                device_id=group_peer(d),
                device_id_type=MESH,
            ).start()

    def final_place(origin, k, core):
        tile, row, rows, _ = UNITS[k]
        at = (origin * 2 + core) * ROWS + row
        if tile < TILES:
            return out_q.at[pl.ds(pl.multiple_of(at, 32), rows), pl.ds(tile * LANES, LANES)]
        return out_kv.at[:, pl.ds(pl.multiple_of(at, HALF), rows)]

    def kv_part(origin, k, last):
        first, columns = (LANES, HALF - LANES) if last else (0, LANES)
        at = origin * 2 * ROWS + UNITS[k][1] + first
        return out_kv.at[:, pl.ds(pl.multiple_of(at, LANES), columns)]

    def place(origin, k):
        _, row, rows, _ = UNITS[k]
        return coded.at[origin, pl.ds(row, rows)] if k < len(CODED) else final_place(origin, k, c)

    def unit_copy(ref, recv_sem, device, sem=send_sem):
        return pltpu.make_async_remote_copy(
            src_ref=ref, dst_ref=ref, send_sem=sem, recv_sem=recv_sem, device_id=device, device_id_type=MESH
        )

    def wait_units(units, sem):
        rows = sum(64 * HALF // LANES if k >= KV_UNITS[0] else UNITS[k][2] for k in units)
        wait_bytes(out_q.at[pl.ds(0, rows), pl.ds(0, LANES)], sem)

    to_right, to_left = {"zero_0": right}, {"zero_0": left}

    def send_right(k):
        unit_copy(place(x, k), side_recv.at[0, SIDE_OF[k]], to_right).start()

    def send_left(k):
        unit_copy(place(x, k), side_recv.at[1, SIDE_OF[k]], to_left).start()

    def relay(origin, k):
        unit_copy(final_place(origin, k, c), rel_recv, partner).start()

    def encode_rows(k, scale):
        _, row, rows, _ = UNITS[k]
        step = STEPS[rows]

        def body(i, carry):
            at = pl.ds(pl.multiple_of(row + i * step, 16), step)
            coded[x, at, :] = encode(res_q[at, 0:LANES], scale)
            return carry

        lax.fori_loop(0, rows // step, body, 0)

    def decode_rows(origin, k, scale):
        _, row, rows, _ = UNITS[k]
        step = STEPS[rows]
        own = sums[origin * 2 + c, MAX_ROW + (k % 3 > 0)] * scale

        def body(i, carry):
            at = pl.multiple_of(row + i * step, 16)
            there = pl.ds(pl.multiple_of((origin * 2 + c) * ROWS + at, 16), step)
            out_q[there, 0:LANES] = (decode(coded[origin, pl.ds(at, step), :]) * own).astype(jnp.bfloat16)
            return carry

        lax.fori_loop(0, rows // step, body, 0)

    lane_of = lax.broadcasted_iota(jnp.int32, (KV, LANES), 1)
    diagonal = lane_of == lax.broadcasted_iota(jnp.int32, (KV, LANES), 0)

    acc, scale = sum_first(0, nothing)
    encode_rows(0, scale)
    encode_rows(3, scale)
    wait_for_neighbours()
    send_right(0)
    send_left(3)
    acc, scale = sum_first(1, acc)
    encode_rows(1, scale)
    send_right(1)
    encode_rows(4, scale)
    send_left(4)
    sum_tile(1)
    wait_for_far()
    send_sums(0, 1, 0)
    encode_rows(2, scale)
    send_right(2)
    encode_rows(5, scale)
    send_left(5)
    sums[me, ROW_OF[0]] = jnp.sum(acc, axis=0, keepdims=True)
    wait_bytes(wq_v.at[pl.ds(0, 4 * 32 * ROWS // COLS), :], in_sem.at[KV_ROW + 1])
    acc = jnp.zeros((KV, LANES), jnp.float32)
    for j in range(ROWS // LANES):
        cols = pl.ds(j * LANES, LANES)
        r = mix(skv_v[:, cols], wkv_v[:, cols])
        res_kv[:, cols] = r
        acc = acc + jnp.abs(r)
    row_sums = jnp.sum(acc, axis=1, keepdims=True)
    sums[me, KV_ROW] = jnp.sum(jnp.where(diagonal, row_sums, 0.0), axis=0, keepdims=True)
    wait_bytes(norm_v, in_sem.at[NORM_ROW + 1])
    own_norm = norm_v[0] + norm_v[1]
    sums[me, NORM_ROW] = jnp.concatenate([own_norm, own_norm], axis=1)
    for t in range(2, TILES):
        sum_tile(t)
    send_sums(1, SUM_ROWS - 1, 1)
    for k in (0, 1, 2):
        send_left(k)
    for k in (3, 4, 5):
        send_right(k)

    def factor_of(t):
        total = sums[0, ROW_OF[t]]
        for other in range(1, 8):
            total = total + sums[other, ROW_OF[t]]
        return total * (1.0 / D_MODEL)

    def narrow_tile(t):
        factor = factor_of(t)
        if t < TILES:
            fac_q[:, pl.ds(t * LANES, LANES)] = factor
            scale = 1.0 / factor
        else:
            fac_k[...] = factor[:, 0:32]
            fac_v[...] = pltpu.roll(factor, LANES - 32, 1)[:, 0:32]
            spread = jnp.sum(jnp.where(diagonal, jnp.broadcast_to(factor, (KV, LANES)), 0.0), axis=1, keepdims=True)
            scale = 1.0 / jnp.broadcast_to(spread, (KV, LANES))
        for half in range(2):
            if t < TILES:
                cols = pl.ds(t * LANES, LANES)

                def body(i, carry):
                    at = half * HALF + i * STEP
                    rows = pl.ds(pl.multiple_of(at, STEP), STEP)
                    there = pl.ds(pl.multiple_of(me * ROWS + at, STEP), STEP)
                    out_q[there, cols] = (res_q[rows, cols] * scale).astype(jnp.bfloat16)
                    return carry

                lax.fori_loop(0, HALF // STEP, body, 0)
            else:
                for j in range(HALF // LANES):
                    at = half * HALF + j * LANES
                    there = pl.ds(pl.multiple_of(me * ROWS + at, LANES), LANES)
                    out_kv[:, there] = (res_kv[:, pl.ds(at, LANES)] * scale).astype(jnp.bfloat16)
            for k in range(FIRST_OF[t], len(UNITS)):
                if UNITS[k][0] == t and UNITS[k][3] == half:
                    for go_there in (send_right, send_left) if half == 0 else (send_left, send_right):
                        go_there(k)
                    relay(x, k)

    wait_bytes(sums.at[pl.ds(0, 7), pl.ds(0, 1)], sum_recv.at[0])
    narrow_tile(1)
    wait_bytes(sums.at[pl.ds(0, 7), pl.ds(1, SUM_ROWS - 1)], sum_recv.at[1])
    for t in range(2, TILES + 1):
        narrow_tile(t)
    first_factor = factor_of(0)
    fac_q[:, 0:LANES] = first_factor
    first_scale = 1.0 / (CODE * first_factor)
    for k in range(len(CODED)):
        decode_rows(x, k, first_scale)
        relay(x, k)

    def norm_copy(buf, at, stage, device):
        return pltpu.make_async_remote_copy(
            src_ref=buf.at[at],
            dst_ref=buf.at[at],
            send_sem=norm_send,
            recv_sem=norm_recv.at[stage],
            device_id=device,
            device_id_type=MESH,
        )

    def norm_along_y():
        pl.semaphore_wait(barrier, 6)
        for other in range(8):
            norm_y[y, pl.ds(other, 1), :] = sums[other, NORM_ROW]
        for d in (2, 1, 3):
            norm_copy(norm_y, y, 0, {"width_1": lax.rem(y + d, 4)}).start()

    def norm_along_z():
        wait_bytes(norm_y.at[pl.ds(0, 3)], norm_recv.at[0])
        low = lax.broadcasted_iota(jnp.int32, (8, LANES), 1) < 64
        norm_z[z, 0] = jnp.where(low, norm_y[0], norm_y[1])
        norm_z[z, 1] = jnp.where(low, norm_y[2], norm_y[3])
        for d in (2, 1, 3):
            norm_copy(norm_z, z, 1, {"width_0": lax.rem(z + d, 4)}).start()

    def norm_end():
        wait_bytes(norm_z.at[pl.ds(0, 3)], norm_recv.at[1])
        for zz in range(4):
            for pair in range(2):
                for other in range(8):
                    norm_all[pl.ds(other * 8 + zz * 2 + pair, 1), :] = norm_z[zz, pair, pl.ds(other, 1), :]
        norm_out[...] = norm_all[...].astype(jnp.bfloat16)

    def norm_give():
        norm_to_partner().start()

    def norm_to_partner():
        return norm_copy(norm_out, pl.ds(0, 64), 2, partner)

    far = lax.rem(x + 2, 4)
    norm_steps = {1: norm_along_y, 2: norm_along_z, 3: norm_end}

    def hand_on(origin, k):
        if k < len(CODED):
            decode_rows(origin, k, first_scale)
        relay(origin, k)

    def forward(origin, k):
        unit_copy(place(origin, k), far_recv.at[FAR_OF[k]], to_left if UNITS[k][3] else to_right).start()

    for i in range(len(SIDE_GROUPS)):
        for side in range(2):
            group = i if i > 1 or side == 0 else 1 - i
            units, origin = SIDE_GROUPS[group], left if side == 0 else right
            wait_units(units, side_recv.at[side, group])
            for k in units:
                if UNITS[k][3] == side and k in KV_UNITS:

                    @pl.when(c == 1)
                    def _():
                        forward(origin, k)
                        relay(origin, k)

                    @pl.when(c == 0)
                    def _():
                        unit_copy(final_place(origin, k, 0), kv_recv, partner).start()
                    continue
                if UNITS[k][3] == side:
                    forward(origin, k)
                hand_on(origin, k)
        if i in norm_steps:
            pl.when(c == 0)(norm_steps[i])

    @pl.when(c == 1)
    def _():
        wait_units(KV_UNITS, kv_recv)
        for side, origin, device in ((0, left, to_right), (1, right, to_left)):
            k = KV_UNITS[side]
            unit_copy(kv_part(origin, k, False), far_kv_recv.at[0], device, extra_send).start()
            for core in range(2):
                to = {**device, "zero_1": core}
                unit_copy(kv_part(origin, k, True), far_kv_recv.at[1], to, extra_send).start()

    pl.when(c == 0)(norm_give)
    pl.when(c == 0)(lambda: wait_bytes(out_q.at[pl.ds(0, 9 * 16 + 64), pl.ds(0, LANES)], norm_send))
    pl.when(c == 1)(lambda: norm_to_partner().wait_recv())
    for group, units in enumerate(FAR_GROUPS):
        if units[0] in KV_UNITS:
            continue
        wait_units(units, far_recv.at[group])
        for k in units:
            hand_on(far, k)

    @pl.when(c == 1)
    def _():
        for k in KV_UNITS:
            wait_units((k,), far_recv.at[FAR_OF[k]])
            relay(far, k)
        wait_bytes(out_kv.at[:, pl.ds(0, 2 * LANES)], far_kv_recv.at[0])
        for k in KV_UNITS:
            unit_copy(kv_part(far, k, False), rel_recv, partner, extra_send).start()

    wait_bytes(out_kv.at[:, pl.ds(0, 2 * (HALF - LANES))], far_kv_recv.at[1])

    share = ROWS + KV * ROWS // COLS
    kv_rows = KV * ROWS // COLS

    wait_bytes(sums.at[pl.ds(0, 7)], sum_send)

    @pl.when(c == 1)
    def _():
        wait_bytes(out_q.at[pl.ds(0, 7 * share), :], send_sem)
        wait_bytes(out_q.at[pl.ds(0, 2 * kv_rows), :], extra_send)
        wait_bytes(out_q.at[pl.ds(0, 4 * share - 2 * kv_rows), :], rel_recv)

    @pl.when(c == 0)
    def _():
        wait_bytes(out_q.at[pl.ds(0, 7 * share - 2 * kv_rows), :], send_sem)
        wait_bytes(out_q.at[pl.ds(0, 4 * share + kv_rows // 4), :], rel_recv)


def write_kernel(
    out_q, out_kv, res_q, res_kv, fac_q, fac_k, fac_v, norm,
    final_q, final_k, final_v, factor_q, factor_k, factor_v, serve_norm, result_q, result_k, result_v, sem,
):
    def write(src, dst, which):
        pltpu.make_async_copy(src, dst, sem.at[which]).start()

    small = ((fac_q, factor_q), (fac_k, factor_k), (fac_v, factor_v), (norm, serve_norm))
    for i, (src, dst) in enumerate(small):
        write(src, dst, i)
    for part in range(8):
        rows = pl.ds(part * ROWS, ROWS)
        write(out_q.at[rows, :], final_q.at[rows, :], 4)
    write(res_q, result_q, 5)
    write(out_kv.at[pl.ds(0, 32), :], final_k, 6)
    write(out_kv.at[pl.ds(32, 32), :], final_v, 6)
    write(res_kv.at[pl.ds(0, 32), :], result_k, 7)
    write(res_kv.at[pl.ds(32, 32), :], result_v, 7)
    for i, ref in enumerate((fac_q, fac_k, fac_v, norm, out_q, res_q, out_kv, res_kv)):
        pltpu.make_async_copy(ref, ref, sem.at[i]).wait()


def on_device(weight_query, smooth_query, weight_key, smooth_key, weight_value, smooth_value, norm_train, norm_step):
    f32, bf16 = jnp.float32, jnp.bfloat16
    any_spec, vmem_spec = pl.BlockSpec(memory_space=pl.ANY), pl.BlockSpec(memory_space=pltpu.VMEM)
    held = (
        ((D_MODEL, COLS), bf16),
        ((KV, D_MODEL), bf16),
        ((ROWS, COLS), f32),
        ((KV, ROWS), f32),
        ((1, COLS), f32),
        ((1, 32), f32),
        ((1, 32), f32),
        ((64, LANES), bf16),
    )
    dma = pltpu.SemaphoreType.DMA
    gathered = pl.pallas_call(
        gather_kernel,
        out_shape=tuple(pltpu.VMEM(shape, dtype) for shape, dtype in held),
        in_specs=[any_spec] * 8,
        out_specs=tuple(vmem_spec for _ in held),
        scratch_shapes=[
            pltpu.VMEM((ROWS, COLS), f32),
            pltpu.VMEM((ROWS, COLS), f32),
            pltpu.VMEM((KV, ROWS), f32),
            pltpu.VMEM((KV, ROWS), f32),
            pltpu.VMEM((2, 1, 64), f32),
            pltpu.VMEM((4, ROWS, LANES), bf16),
            pltpu.VMEM((8, SUM_ROWS, 1, LANES), f32),
            pltpu.VMEM((4, 8, LANES), f32),
            pltpu.VMEM((4, 2, 8, LANES), f32),
            pltpu.VMEM((64, LANES), f32),
            dma((NORM_ROW + 2,)),
            dma,
            dma,
            dma,
            dma((2,)),
            dma((2, len(SIDE_GROUPS))),
            dma((len(FAR_GROUPS),)),
            dma,
            dma,
            dma((2,)),
            dma,
            dma((3,)),
            pltpu.SemaphoreType.REGULAR((2,)),
            pltpu.SemaphoreType.REGULAR,
        ],
        compiler_params=pltpu.CompilerParams(
            collective_id=0, has_side_effects=True, vmem_limit_bytes=16 * 1024 * 1024
        ),
        name="gather",
    )(
        *(
            pltpu.with_memory_space_constraint(a, pltpu.HBM)
            for a in (
                weight_query, smooth_query, weight_key.T, smooth_key.T, weight_value.T, smooth_value.T,
                norm_train.reshape(1, 64), norm_step.reshape(1, 64),
            )
        )
    )
    outs = (
        ((D_MODEL, COLS), bf16),
        ((32, D_MODEL), bf16),
        ((32, D_MODEL), bf16),
        ((1, COLS), f32),
        ((1, 32), f32),
        ((1, 32), f32),
        ((64, LANES), bf16),
        ((ROWS, COLS), f32),
        ((32, ROWS), f32),
        ((32, ROWS), f32),
    )
    fq, fk, fv, cq, ck, cv, norm, rq, rk, rv = pl.pallas_call(
        write_kernel,
        out_shape=tuple(jax.ShapeDtypeStruct(shape, dtype) for shape, dtype in outs),
        in_specs=[vmem_spec] * len(held),
        out_specs=tuple(any_spec for _ in outs),
        scratch_shapes=[dma((8,))],
        compiler_params=pltpu.CompilerParams(vmem_limit_bytes=4 * 1024 * 1024),
        name="write",
    )(*gathered)
    return (
        fq, fk.T, fv.T, cq.reshape(COLS), ck.reshape(32), cv.reshape(32), norm.reshape(D_MODEL), rq, rk.T, rv.T
    )


def solution(mesh):
    split = Mesh(mesh.devices.reshape(4, 2, 4, 4), ("zero_0", "zero_1", "width_0", "width_1"))
    in_specs = (
        P(ZERO, WIDTH),
        P(ZERO, WIDTH),
        P(ZERO, WIDTH),
        P(ZERO, WIDTH),
        P(ZERO, WIDTH),
        P(ZERO, WIDTH),
        P(ZERO_WIDTH),
        P(ZERO_WIDTH),
    )
    out_specs = (
        P(None, WIDTH),
        P(None, WIDTH),
        P(None, WIDTH),
        P(WIDTH),
        P(WIDTH),
        P(WIDTH),
        P(),
        P(ZERO, WIDTH),
        P(ZERO, WIDTH),
        P(ZERO, WIDTH),
    )
    return jax.shard_map(
        on_device, mesh=split, in_specs=in_specs, out_specs=out_specs, check_vma=False
    )
```

```python
import jax
import jax.numpy as jnp
from jax import lax
from jax.experimental import pallas as pl
from jax.experimental.pallas import tpu as pltpu
from jax.sharding import Mesh
from jax.sharding import PartitionSpec as P

D_MODEL = 8192
ZERO = ("zero_0", "zero_1")
ZERO_WIDTH = ("zero_0", "zero_1", "width_0", "width_1")
WIDTH = ("width_0", "width_1")
MESH = pl.DeviceIdType.MESH

keep_rate = 0.7

ROWS = 1024
COLS = 512
HALF = ROWS // 2
KV = 64
LANES = 128
TILES = COLS // LANES
STEP = 128
KV_ROW, NORM_ROW, MAX_ROW = TILES, TILES + 1, TILES + 2
SUM_ROWS = TILES + 5

FIRST = 128
CODED_TILES = 2
CODED = (
    *((0, half * HALF + row, rows, half) for half in range(2) for row, rows in ((0, FIRST), (FIRST, HALF - FIRST))),
    *((1, half * HALF, HALF, half) for half in range(2)),
)
QUARTER = HALF // 2
UNITS = (
    *CODED,
    *((tile, half * HALF, HALF, half) for tile in range(CODED_TILES, TILES - 1) for half in range(2)),
    *((TILES - 1, part * QUARTER, QUARTER, part // 2) for part in range(4)),
    *((TILES, half * HALF, HALF, half) for half in range(2)),
)
FIRST_OF = tuple(min(k for k, unit in enumerate(UNITS) if unit[0] == tile) for tile in range(TILES + 1))
KV_UNITS = (len(UNITS) - 2, len(UNITS) - 1)
SIDE_GROUPS = ((0, 1), (2, 3), (4, 5, 6, 7), (8, 9, 10, 11, 12, 13))
FAR_GROUPS = ((0, 1), (2, 3), (4, 6), (5, 7), (8,), (10,), (9,), (11,), (12,), (13,))
SIDE_OF = {k: g for g, units in enumerate(SIDE_GROUPS) for k in units}
FAR_OF = {k: g for g, units in enumerate(FAR_GROUPS) for k in units}
CODE = 180.0


def mix(smooth, weight):
    return keep_rate * smooth + (1.0 - keep_rate) * weight


def encode(x, scale):
    v = x * scale
    for _ in range(4):
        v = v * v
    return jnp.where(x < 0, -v, v).astype(jnp.bfloat16)


def decode(code):
    v = code.astype(jnp.float32)
    root = jnp.abs(v)
    for _ in range(4):
        root = lax.rsqrt(root)
    return jnp.where(v < 0, -root, root)


def gather_kernel(
    wq, sq, wk, sk, wv, sv, norm_a, norm_b,
    out_q, out_kv, res_q, res_kv, fac_q, fac_k, fac_v, norm_out,
    wq_v, sq_v, wkv_v, skv_v, norm_v, coded, sums, norm_y, norm_z, norm_all,
    in_sem, send_sem, extra_send, sum_send, sum_recv, side_recv, far_recv, rel_recv, kv_recv, far_kv_recv,
    norm_send, norm_recv, go, vouch,
):
    x, c = lax.axis_index("zero_0"), lax.axis_index("zero_1")
    z, y = lax.axis_index("width_0"), lax.axis_index("width_1")
    me = x * 2 + c
    right, left = lax.rem(x + 1, 4), lax.rem(x + 3, 4)
    partner = {"zero_1": 1 - c}

    def load(src, dst, which):
        pltpu.make_async_copy(src, dst, in_sem.at[which]).start()

    def load_rows(t, first, rows, which):
        at = (pl.ds(first, rows), pl.ds(t * LANES, LANES))
        load(wq.at[at], wq_v.at[at], which)
        load(sq.at[at], sq_v.at[at], which)

    def wait_bytes(ref, sem):
        pltpu.make_async_copy(ref, ref, sem).wait()

    barrier = pltpu.get_barrier_semaphore()
    for device in ({"zero_0": right, "zero_1": 1}, {"zero_0": left, "zero_1": 1}):
        pl.semaphore_signal(barrier, inc=1, device_id=device, device_id_type=MESH)

    @pl.when(c == 0)
    def _():
        pl.semaphore_signal(barrier, inc=1, device_id=partner, device_id_type=MESH)

    for row in (0, HALF):
        load_rows(0, row, FIRST, 0)
    for row in (FIRST, HALF + FIRST):
        load_rows(0, row, HALF - FIRST, TILES)
    load_rows(1, 0, ROWS, 1)
    load(wk, wkv_v.at[pl.ds(0, 32), :], KV_ROW + 1)
    load(sk, skv_v.at[pl.ds(0, 32), :], KV_ROW + 1)
    load(wv, wkv_v.at[pl.ds(32, 32), :], KV_ROW + 1)
    load(sv, skv_v.at[pl.ds(32, 32), :], KV_ROW + 1)
    load(norm_a, norm_v.at[0], NORM_ROW + 1)
    load(norm_b, norm_v.at[1], NORM_ROW + 1)
    for t in range(2, TILES):
        load_rows(t, 0, ROWS, t)

    @pl.when(c == 0)
    def _():
        for d in (2, 1, 3):
            pl.semaphore_signal(barrier, inc=1, device_id={"width_1": lax.rem(y + d, 4)}, device_id_type=MESH)
            pl.semaphore_signal(barrier, inc=1, device_id={"width_0": lax.rem(z + d, 4)}, device_id_type=MESH)

    def wait_for_neighbours():
        @pl.when(c == 1)
        def _():
            pl.semaphore_wait(barrier, 5)
            pl.semaphore_signal(go.at[0], inc=1, device_id=partner, device_id_type=MESH)
            for side in (left, right):
                pl.semaphore_signal(vouch, inc=1, device_id={"zero_0": side}, device_id_type=MESH)

        @pl.when(c == 0)
        def _():
            pl.semaphore_wait(go.at[0], 1)

    def wait_for_far():
        @pl.when(c == 1)
        def _():
            pl.semaphore_wait(vouch, 2)
            pl.semaphore_signal(go.at[1], inc=1, device_id=partner, device_id_type=MESH)

        @pl.when(c == 0)
        def _():
            pl.semaphore_wait(go.at[1], 1)

    def group_peer(d):
        other = lax.rem(me + d, 8)
        return {"zero_0": other // 2, "zero_1": lax.rem(other, 2)}

    nothing = jnp.zeros((8, LANES), jnp.float32)

    def sum_rows(t, first, rows, carry):
        cols = pl.ds(t * LANES, LANES)

        def body(i, carry):
            acc, top = carry
            at = pl.ds(pl.multiple_of(first + i * STEP, STEP), STEP)
            r = mix(sq_v[at, cols], wq_v[at, cols])
            res_q[at, cols] = r
            size = jnp.abs(r).reshape(STEP // 8, 8, LANES)
            acc = acc + jnp.sum(size, axis=0)
            return acc, jnp.maximum(top, jnp.max(size, axis=0)) if t < CODED_TILES else top

        return lax.fori_loop(0, rows // STEP, body, carry)

    def code_scale(top, row):
        top = jnp.maximum(jnp.max(top, axis=0, keepdims=True), 1e-30)
        sums[me, MAX_ROW + row] = top
        return CODE / top

    def sum_tile(t):
        wait_bytes(wq_v.at[:, pl.ds(0, 2 * LANES)], in_sem.at[t])
        acc, top = sum_rows(t, 0, ROWS, (nothing, nothing))
        sums[me, t] = jnp.sum(acc, axis=0, keepdims=True)
        return code_scale(top, 2) if t < CODED_TILES else None

    def sum_first(part, acc):
        row, rows = (0, FIRST) if part == 0 else (FIRST, HALF - FIRST)
        wait_bytes(wq_v.at[pl.ds(0, rows), :], in_sem.at[part * TILES])
        carry = (acc, nothing)
        for half in range(2):
            carry = sum_rows(0, half * HALF + row, rows, carry)
        acc, top = carry
        return acc, code_scale(top, part)

    def send_sums():
        for d in (4, 5, 3, 2, 6, 7, 1):
            pltpu.make_async_remote_copy(
                src_ref=sums.at[me],
                dst_ref=sums.at[me],
                send_sem=sum_send,
                recv_sem=sum_recv,
                device_id=group_peer(d),
                device_id_type=MESH,
            ).start()

    def final_place(origin, k, core):
        tile, row, rows, _ = UNITS[k]
        at = (origin * 2 + core) * ROWS + row
        if tile < TILES:
            return out_q.at[pl.ds(pl.multiple_of(at, STEP), rows), pl.ds(tile * LANES, LANES)]
        return out_kv.at[:, pl.ds(pl.multiple_of(at, HALF), rows)]

    def kv_part(origin, k, last):
        first, columns = (LANES, HALF - LANES) if last else (0, LANES)
        at = origin * 2 * ROWS + UNITS[k][1] + first
        return out_kv.at[:, pl.ds(pl.multiple_of(at, LANES), columns)]

    def place(origin, k):
        tile, row, rows, _ = UNITS[k]
        return coded.at[origin, tile, pl.ds(row, rows)] if k < len(CODED) else final_place(origin, k, c)

    def unit_copy(ref, recv_sem, device, sem=send_sem):
        return pltpu.make_async_remote_copy(
            src_ref=ref, dst_ref=ref, send_sem=sem, recv_sem=recv_sem, device_id=device, device_id_type=MESH
        )

    def wait_units(units, sem):
        rows = sum(64 * HALF // LANES if k >= KV_UNITS[0] else UNITS[k][2] for k in units)
        wait_bytes(out_q.at[pl.ds(0, rows), pl.ds(0, LANES)], sem)

    to_right, to_left = {"zero_0": right}, {"zero_0": left}

    def send_right(k):
        unit_copy(place(x, k), side_recv.at[0, SIDE_OF[k]], to_right).start()

    def send_left(k):
        unit_copy(place(x, k), side_recv.at[1, SIDE_OF[k]], to_left).start()

    def relay(origin, k):
        unit_copy(final_place(origin, k, c), rel_recv, partner).start()

    def encode_rows(k, scale):
        tile, row, rows, _ = UNITS[k]
        cols = pl.ds(tile * LANES, LANES)

        def body(i, carry):
            at = pl.ds(pl.multiple_of(row + i * STEP, STEP), STEP)
            coded[x, tile, at, :] = encode(res_q[at, cols], scale)
            return carry

        lax.fori_loop(0, rows // STEP, body, 0)

    def decode_rows(origin, k, scales):
        tile, row, rows, _ = UNITS[k]
        cols = pl.ds(tile * LANES, LANES)
        own = sums[origin * 2 + c, MAX_ROW + (2 if tile else int(rows != FIRST))] * scales[tile]

        def body(i, carry):
            at = pl.multiple_of(row + i * STEP, STEP)
            there = pl.ds(pl.multiple_of((origin * 2 + c) * ROWS + at, STEP), STEP)
            out_q[there, cols] = (decode(coded[origin, tile, pl.ds(at, STEP), :]) * own).astype(jnp.bfloat16)
            return carry

        lax.fori_loop(0, rows // STEP, body, 0)

    lane_of = lax.broadcasted_iota(jnp.int32, (KV, LANES), 1)
    diagonal = lane_of == lax.broadcasted_iota(jnp.int32, (KV, LANES), 0)

    acc, scale = sum_first(0, nothing)
    encode_rows(0, scale)
    encode_rows(2, scale)
    wait_for_neighbours()
    send_right(0)
    send_left(2)
    acc, scale = sum_first(1, acc)
    encode_rows(1, scale)
    send_right(1)
    encode_rows(3, scale)
    for k in (3, 0, 1):
        send_left(k)
    for k in (2, 3):
        send_right(k)
    sums[me, 0] = jnp.sum(acc, axis=0, keepdims=True)
    scale = sum_tile(1)
    wait_bytes(wq_v.at[pl.ds(0, 4 * 32 * ROWS // COLS), :], in_sem.at[KV_ROW + 1])
    acc = jnp.zeros((KV, LANES), jnp.float32)
    for j in range(ROWS // LANES):
        cols = pl.ds(j * LANES, LANES)
        r = mix(skv_v[:, cols], wkv_v[:, cols])
        res_kv[:, cols] = r
        acc = acc + jnp.abs(r)
    row_sums = jnp.sum(acc, axis=1, keepdims=True)
    sums[me, KV_ROW] = jnp.sum(jnp.where(diagonal, row_sums, 0.0), axis=0, keepdims=True)
    wait_bytes(norm_v, in_sem.at[NORM_ROW + 1])
    own_norm = norm_v[0] + norm_v[1]
    sums[me, NORM_ROW] = jnp.concatenate([own_norm, own_norm], axis=1)
    for t in range(2, TILES):
        sum_tile(t)
    wait_for_far()
    send_sums()
    encode_rows(4, scale)
    encode_rows(5, scale)
    for k in (4, 5):
        send_right(k)
    for k in (5, 4):
        send_left(k)

    def factor_of(t):
        total = sums[0, t]
        for other in range(1, 8):
            total = total + sums[other, t]
        return total * (1.0 / D_MODEL)

    def narrow_tile(t):
        factor = factor_of(t)
        if t < TILES:
            fac_q[:, pl.ds(t * LANES, LANES)] = factor
            scale = 1.0 / factor
        else:
            fac_k[...] = factor[:, 0:32]
            fac_v[...] = pltpu.roll(factor, LANES - 32, 1)[:, 0:32]
            spread = jnp.sum(jnp.where(diagonal, jnp.broadcast_to(factor, (KV, LANES)), 0.0), axis=1, keepdims=True)
            scale = 1.0 / jnp.broadcast_to(spread, (KV, LANES))
        for half in range(2):
            if t < TILES:
                cols = pl.ds(t * LANES, LANES)

                def body(i, carry):
                    at = half * HALF + i * STEP
                    rows = pl.ds(pl.multiple_of(at, STEP), STEP)
                    there = pl.ds(pl.multiple_of(me * ROWS + at, STEP), STEP)
                    out_q[there, cols] = (res_q[rows, cols] * scale).astype(jnp.bfloat16)
                    return carry

                lax.fori_loop(0, HALF // STEP, body, 0)
            else:
                for j in range(HALF // LANES):
                    at = half * HALF + j * LANES
                    there = pl.ds(pl.multiple_of(me * ROWS + at, LANES), LANES)
                    out_kv[:, there] = (res_kv[:, pl.ds(at, LANES)] * scale).astype(jnp.bfloat16)
            for k in range(FIRST_OF[t], len(UNITS)):
                if UNITS[k][0] == t and UNITS[k][3] == half:
                    for go_there in (send_right, send_left) if half == 0 else (send_left, send_right):
                        go_there(k)
                    relay(x, k)

    wait_bytes(sums.at[pl.ds(0, 7)], sum_recv)
    for t in range(CODED_TILES, TILES + 1):
        narrow_tile(t)
    scales = []
    for t in range(CODED_TILES):
        factor = factor_of(t)
        fac_q[:, pl.ds(t * LANES, LANES)] = factor
        scales.append(1.0 / (CODE * factor))
    for k in range(len(CODED)):
        decode_rows(x, k, scales)
        relay(x, k)

    def norm_copy(buf, at, stage, device):
        return pltpu.make_async_remote_copy(
            src_ref=buf.at[at],
            dst_ref=buf.at[at],
            send_sem=norm_send,
            recv_sem=norm_recv.at[stage],
            device_id=device,
            device_id_type=MESH,
        )

    def norm_along_y():
        pl.semaphore_wait(barrier, 6)
        for other in range(8):
            norm_y[y, pl.ds(other, 1), :] = sums[other, NORM_ROW]
        for d in (2, 1, 3):
            norm_copy(norm_y, y, 0, {"width_1": lax.rem(y + d, 4)}).start()

    def norm_along_z():
        wait_bytes(norm_y.at[pl.ds(0, 3)], norm_recv.at[0])
        low = lax.broadcasted_iota(jnp.int32, (8, LANES), 1) < 64
        norm_z[z, 0] = jnp.where(low, norm_y[0], norm_y[1])
        norm_z[z, 1] = jnp.where(low, norm_y[2], norm_y[3])
        for d in (2, 1, 3):
            norm_copy(norm_z, z, 1, {"width_0": lax.rem(z + d, 4)}).start()

    def norm_end():
        wait_bytes(norm_z.at[pl.ds(0, 3)], norm_recv.at[1])
        for zz in range(4):
            for pair in range(2):
                for other in range(8):
                    norm_all[pl.ds(other * 8 + zz * 2 + pair, 1), :] = norm_z[zz, pair, pl.ds(other, 1), :]
        norm_out[...] = norm_all[...].astype(jnp.bfloat16)

    def norm_give():
        norm_to_partner().start()

    def norm_to_partner():
        return norm_copy(norm_out, pl.ds(0, 64), 2, partner)

    far = lax.rem(x + 2, 4)
    norm_steps = {1: norm_along_y, 2: norm_along_z, 3: norm_end}

    def hand_on(origin, k):
        if k < len(CODED):
            decode_rows(origin, k, scales)
        relay(origin, k)

    def forward(origin, k):
        unit_copy(place(origin, k), far_recv.at[FAR_OF[k]], to_left if UNITS[k][3] else to_right).start()

    for i in range(len(SIDE_GROUPS)):
        for side in range(2):
            group = i if i > 1 or side == 0 else 1 - i
            units, origin = SIDE_GROUPS[group], left if side == 0 else right
            wait_units(units, side_recv.at[side, group])
            for k in units:
                if UNITS[k][3] == side and k in KV_UNITS:

                    @pl.when(c == 1)
                    def _():
                        forward(origin, k)
                        relay(origin, k)

                    @pl.when(c == 0)
                    def _():
                        unit_copy(final_place(origin, k, 0), kv_recv, partner).start()
                    continue
                if UNITS[k][3] == side:
                    forward(origin, k)
                hand_on(origin, k)
        if i in norm_steps:
            pl.when(c == 0)(norm_steps[i])

    @pl.when(c == 1)
    def _():
        wait_units(KV_UNITS, kv_recv)
        for side, origin, device in ((0, left, to_right), (1, right, to_left)):
            k = KV_UNITS[side]
            unit_copy(kv_part(origin, k, False), far_kv_recv.at[0], device, extra_send).start()
            for core in range(2):
                to = {**device, "zero_1": core}
                unit_copy(kv_part(origin, k, True), far_kv_recv.at[1], to, extra_send).start()

    pl.when(c == 0)(norm_give)
    pl.when(c == 0)(lambda: wait_bytes(out_q.at[pl.ds(0, 9 * 16 + 64), pl.ds(0, LANES)], norm_send))
    pl.when(c == 1)(lambda: norm_to_partner().wait_recv())
    for group, units in enumerate(FAR_GROUPS):
        if units[0] in KV_UNITS:
            continue
        wait_units(units, far_recv.at[group])
        for k in units:
            hand_on(far, k)

    @pl.when(c == 1)
    def _():
        for k in KV_UNITS:
            wait_units((k,), far_recv.at[FAR_OF[k]])
            relay(far, k)
        wait_bytes(out_kv.at[:, pl.ds(0, 2 * LANES)], far_kv_recv.at[0])
        for k in KV_UNITS:
            unit_copy(kv_part(far, k, False), rel_recv, partner, extra_send).start()

    wait_bytes(out_kv.at[:, pl.ds(0, 2 * (HALF - LANES))], far_kv_recv.at[1])

    share = ROWS + KV * ROWS // COLS
    kv_rows = KV * ROWS // COLS

    wait_bytes(sums.at[pl.ds(0, 7)], sum_send)

    @pl.when(c == 1)
    def _():
        wait_bytes(out_q.at[pl.ds(0, 7 * share), :], send_sem)
        wait_bytes(out_q.at[pl.ds(0, 2 * kv_rows), :], extra_send)
        wait_bytes(out_q.at[pl.ds(0, 4 * share - 2 * kv_rows), :], rel_recv)

    @pl.when(c == 0)
    def _():
        wait_bytes(out_q.at[pl.ds(0, 7 * share - 2 * kv_rows), :], send_sem)
        wait_bytes(out_q.at[pl.ds(0, 4 * share + kv_rows // 4), :], rel_recv)


def write_kernel(
    out_q, out_kv, res_q, res_kv, fac_q, fac_k, fac_v, norm,
    final_q, final_k, final_v, factor_q, factor_k, factor_v, serve_norm, result_q, result_k, result_v, sem,
):
    def write(src, dst, which):
        pltpu.make_async_copy(src, dst, sem.at[which]).start()

    small = ((fac_q, factor_q), (fac_k, factor_k), (fac_v, factor_v), (norm, serve_norm))
    for i, (src, dst) in enumerate(small):
        write(src, dst, i)
    for part in range(8):
        rows = pl.ds(part * ROWS, ROWS)
        write(out_q.at[rows, :], final_q.at[rows, :], 4)
    write(res_q, result_q, 5)
    write(out_kv.at[pl.ds(0, 32), :], final_k, 6)
    write(out_kv.at[pl.ds(32, 32), :], final_v, 6)
    write(res_kv.at[pl.ds(0, 32), :], result_k, 7)
    write(res_kv.at[pl.ds(32, 32), :], result_v, 7)
    for i, ref in enumerate((fac_q, fac_k, fac_v, norm, out_q, res_q, out_kv, res_kv)):
        pltpu.make_async_copy(ref, ref, sem.at[i]).wait()


def on_device(weight_query, smooth_query, weight_key, smooth_key, weight_value, smooth_value, norm_train, norm_step):
    f32, bf16 = jnp.float32, jnp.bfloat16
    any_spec, vmem_spec = pl.BlockSpec(memory_space=pl.ANY), pl.BlockSpec(memory_space=pltpu.VMEM)
    held = (
        ((D_MODEL, COLS), bf16),
        ((KV, D_MODEL), bf16),
        ((ROWS, COLS), f32),
        ((KV, ROWS), f32),
        ((1, COLS), f32),
        ((1, 32), f32),
        ((1, 32), f32),
        ((64, LANES), bf16),
    )
    dma = pltpu.SemaphoreType.DMA
    gathered = pl.pallas_call(
        gather_kernel,
        out_shape=tuple(pltpu.VMEM(shape, dtype) for shape, dtype in held),
        in_specs=[any_spec] * 8,
        out_specs=tuple(vmem_spec for _ in held),
        scratch_shapes=[
            pltpu.VMEM((ROWS, COLS), f32),
            pltpu.VMEM((ROWS, COLS), f32),
            pltpu.VMEM((KV, ROWS), f32),
            pltpu.VMEM((KV, ROWS), f32),
            pltpu.VMEM((2, 1, 64), f32),
            pltpu.VMEM((4, CODED_TILES, ROWS, LANES), bf16),
            pltpu.VMEM((8, SUM_ROWS, 1, LANES), f32),
            pltpu.VMEM((4, 8, LANES), f32),
            pltpu.VMEM((4, 2, 8, LANES), f32),
            pltpu.VMEM((64, LANES), f32),
            dma((NORM_ROW + 2,)),
            dma,
            dma,
            dma,
            dma,
            dma((2, len(SIDE_GROUPS))),
            dma((len(FAR_GROUPS),)),
            dma,
            dma,
            dma((2,)),
            dma,
            dma((3,)),
            pltpu.SemaphoreType.REGULAR((2,)),
            pltpu.SemaphoreType.REGULAR,
        ],
        compiler_params=pltpu.CompilerParams(
            collective_id=0, has_side_effects=True, vmem_limit_bytes=16 * 1024 * 1024
        ),
        name="gather",
    )(
        *(
            pltpu.with_memory_space_constraint(a, pltpu.HBM)
            for a in (
                weight_query, smooth_query, weight_key.T, smooth_key.T, weight_value.T, smooth_value.T,
                norm_train.reshape(1, 64), norm_step.reshape(1, 64),
            )
        )
    )
    outs = (
        ((D_MODEL, COLS), bf16),
        ((32, D_MODEL), bf16),
        ((32, D_MODEL), bf16),
        ((1, COLS), f32),
        ((1, 32), f32),
        ((1, 32), f32),
        ((64, LANES), bf16),
        ((ROWS, COLS), f32),
        ((32, ROWS), f32),
        ((32, ROWS), f32),
    )
    fq, fk, fv, cq, ck, cv, norm, rq, rk, rv = pl.pallas_call(
        write_kernel,
        out_shape=tuple(jax.ShapeDtypeStruct(shape, dtype) for shape, dtype in outs),
        in_specs=[vmem_spec] * len(held),
        out_specs=tuple(any_spec for _ in outs),
        scratch_shapes=[dma((8,))],
        compiler_params=pltpu.CompilerParams(vmem_limit_bytes=4 * 1024 * 1024),
        name="write",
    )(*gathered)
    return (
        fq, fk.T, fv.T, cq.reshape(COLS), ck.reshape(32), cv.reshape(32), norm.reshape(D_MODEL), rq, rk.T, rv.T
    )


def solution(mesh):
    split = Mesh(mesh.devices.reshape(4, 2, 4, 4), ("zero_0", "zero_1", "width_0", "width_1"))
    in_specs = (
        P(ZERO, WIDTH),
        P(ZERO, WIDTH),
        P(ZERO, WIDTH),
        P(ZERO, WIDTH),
        P(ZERO, WIDTH),
        P(ZERO, WIDTH),
        P(ZERO_WIDTH),
        P(ZERO_WIDTH),
    )
    out_specs = (
        P(None, WIDTH),
        P(None, WIDTH),
        P(None, WIDTH),
        P(WIDTH),
        P(WIDTH),
        P(WIDTH),
        P(),
        P(ZERO, WIDTH),
        P(ZERO, WIDTH),
        P(ZERO, WIDTH),
    )
    return jax.shard_map(
        on_device, mesh=split, in_specs=in_specs, out_specs=out_specs, check_vma=False
    )
```

```python
import jax
import jax.numpy as jnp
from jax import lax
from jax.experimental import pallas as pl
from jax.experimental.pallas import tpu as pltpu
from jax.sharding import Mesh
from jax.sharding import PartitionSpec as P

D_MODEL = 8192
ZERO = ("zero_0", "zero_1")
ZERO_WIDTH = ("zero_0", "zero_1", "width_0", "width_1")
WIDTH = ("width_0", "width_1")
MESH = pl.DeviceIdType.MESH

keep_rate = 0.7

ROWS = 1024
COLS = 512
HALF = ROWS // 2
KV = 64
LANES = 128
TILES = COLS // LANES
STEP = 128
KV_ROW, NORM_ROW, MAX_ROW = TILES, TILES + 1, TILES + 2
SUM_ROWS = TILES + 5

FIRST = 128
CODED_TILES = 2
CODED = (
    *((0, half * HALF + row, rows, half) for half in range(2) for row, rows in ((0, FIRST), (FIRST, HALF - FIRST))),
    *((1, half * HALF, HALF, half) for half in range(2)),
)
LAST = 128
UNITS = (
    *CODED,
    *((tile, half * HALF, HALF, half) for tile in range(CODED_TILES, TILES - 1) for half in range(2)),
    *((TILES - 1, half * HALF + row, rows, half) for half in range(2) for row, rows in ((0, HALF - LAST), (HALF - LAST, LAST))),
    *((TILES, half * HALF, HALF, half) for half in range(2)),
)
FIRST_OF = tuple(min(k for k, unit in enumerate(UNITS) if unit[0] == tile) for tile in range(TILES + 1))
KV_UNITS = (len(UNITS) - 2, len(UNITS) - 1)
SIDE_GROUPS = ((0, 1), (2, 3), (4, 5, 6, 7), (8, 9, 10, 11, 12, 13))
FAR_GROUPS = ((0, 1), (2, 3), (4, 6), (5, 7), (8,), (10,), (9,), (11,), (12,), (13,))
SIDE_OF = {k: g for g, units in enumerate(SIDE_GROUPS) for k in units}
FAR_OF = {k: g for g, units in enumerate(FAR_GROUPS) for k in units}
CODE = 180.0


def mix(smooth, weight):
    return keep_rate * smooth + (1.0 - keep_rate) * weight


def encode(x, scale):
    v = x * scale
    for _ in range(4):
        v = v * v
    return jnp.where(x < 0, -v, v).astype(jnp.bfloat16)


def decode(code):
    v = code.astype(jnp.float32)
    root = jnp.abs(v)
    for _ in range(4):
        root = lax.rsqrt(root)
    return jnp.where(v < 0, -root, root)


def gather_kernel(
    wq, sq, wk, sk, wv, sv, norm_a, norm_b,
    out_q, out_kv, res_q, res_kv, fac_q, fac_k, fac_v, norm_out,
    wq_v, sq_v, wkv_v, skv_v, norm_v, coded, sums, norm_y, norm_z, norm_all,
    in_sem, send_sem, extra_send, sum_send, sum_recv, side_recv, far_recv, rel_recv, kv_recv, far_kv_recv,
    norm_send, norm_recv, go, vouch,
):
    x, c = lax.axis_index("zero_0"), lax.axis_index("zero_1")
    z, y = lax.axis_index("width_0"), lax.axis_index("width_1")
    me = x * 2 + c
    right, left = lax.rem(x + 1, 4), lax.rem(x + 3, 4)
    partner = {"zero_1": 1 - c}

    def load(src, dst, which):
        pltpu.make_async_copy(src, dst, in_sem.at[which]).start()

    def load_rows(t, first, rows, which):
        at = (pl.ds(first, rows), pl.ds(t * LANES, LANES))
        load(wq.at[at], wq_v.at[at], which)
        load(sq.at[at], sq_v.at[at], which)

    def wait_bytes(ref, sem):
        pltpu.make_async_copy(ref, ref, sem).wait()

    barrier = pltpu.get_barrier_semaphore()
    for device in ({"zero_0": right, "zero_1": 1}, {"zero_0": left, "zero_1": 1}):
        pl.semaphore_signal(barrier, inc=1, device_id=device, device_id_type=MESH)

    @pl.when(c == 0)
    def _():
        pl.semaphore_signal(barrier, inc=1, device_id=partner, device_id_type=MESH)

    for row in (0, HALF):
        load_rows(0, row, FIRST, 0)
    for row in (FIRST, HALF + FIRST):
        load_rows(0, row, HALF - FIRST, TILES)
    load_rows(1, 0, ROWS, 1)
    load(wk, wkv_v.at[pl.ds(0, 32), :], KV_ROW + 1)
    load(sk, skv_v.at[pl.ds(0, 32), :], KV_ROW + 1)
    load(wv, wkv_v.at[pl.ds(32, 32), :], KV_ROW + 1)
    load(sv, skv_v.at[pl.ds(32, 32), :], KV_ROW + 1)
    load(norm_a, norm_v.at[0], NORM_ROW + 1)
    load(norm_b, norm_v.at[1], NORM_ROW + 1)
    for t in range(2, TILES):
        load_rows(t, 0, ROWS, t)

    @pl.when(c == 0)
    def _():
        for d in (2, 1, 3):
            pl.semaphore_signal(barrier, inc=1, device_id={"width_1": lax.rem(y + d, 4)}, device_id_type=MESH)
            pl.semaphore_signal(barrier, inc=1, device_id={"width_0": lax.rem(z + d, 4)}, device_id_type=MESH)

    def wait_for_neighbours():
        @pl.when(c == 1)
        def _():
            pl.semaphore_wait(barrier, 5)
            pl.semaphore_signal(go.at[0], inc=1, device_id=partner, device_id_type=MESH)
            for side in (left, right):
                pl.semaphore_signal(vouch, inc=1, device_id={"zero_0": side}, device_id_type=MESH)

        @pl.when(c == 0)
        def _():
            pl.semaphore_wait(go.at[0], 1)

    def wait_for_far():
        @pl.when(c == 1)
        def _():
            pl.semaphore_wait(vouch, 2)
            pl.semaphore_signal(go.at[1], inc=1, device_id=partner, device_id_type=MESH)

        @pl.when(c == 0)
        def _():
            pl.semaphore_wait(go.at[1], 1)

    def group_peer(d):
        other = lax.rem(me + d, 8)
        return {"zero_0": other // 2, "zero_1": lax.rem(other, 2)}

    nothing = jnp.zeros((8, LANES), jnp.float32)

    def sum_rows(t, first, rows, carry):
        cols = pl.ds(t * LANES, LANES)

        def body(i, carry):
            acc, top = carry
            at = pl.ds(pl.multiple_of(first + i * STEP, STEP), STEP)
            r = mix(sq_v[at, cols], wq_v[at, cols])
            res_q[at, cols] = r
            size = jnp.abs(r).reshape(STEP // 8, 8, LANES)
            acc = acc + jnp.sum(size, axis=0)
            return acc, jnp.maximum(top, jnp.max(size, axis=0)) if t < CODED_TILES else top

        return lax.fori_loop(0, rows // STEP, body, carry)

    def code_scale(top, row):
        top = jnp.maximum(jnp.max(top, axis=0, keepdims=True), 1e-30)
        sums[me, MAX_ROW + row] = top
        return CODE / top

    def sum_tile(t):
        wait_bytes(wq_v.at[:, pl.ds(0, 2 * LANES)], in_sem.at[t])
        acc, top = sum_rows(t, 0, ROWS, (nothing, nothing))
        sums[me, t] = jnp.sum(acc, axis=0, keepdims=True)
        return code_scale(top, 2) if t < CODED_TILES else None

    def sum_first(part, acc):
        row, rows = (0, FIRST) if part == 0 else (FIRST, HALF - FIRST)
        wait_bytes(wq_v.at[pl.ds(0, rows), :], in_sem.at[part * TILES])
        carry = (acc, nothing)
        for half in range(2):
            carry = sum_rows(0, half * HALF + row, rows, carry)
        acc, top = carry
        return acc, code_scale(top, part)

    def send_sums():
        for d in (4, 5, 3, 2, 6, 7, 1):
            same = d % 2 == 0
            rows = pl.ds(0, SUM_ROWS if same else MAX_ROW)
            pltpu.make_async_remote_copy(
                src_ref=sums.at[me, rows],
                dst_ref=sums.at[me, rows],
                send_sem=sum_send.at[int(same)],
                recv_sem=sum_recv.at[int(same)],
                device_id=group_peer(d),
                device_id_type=MESH,
            ).start()

    def wait_sums(sem):
        wait_bytes(sums.at[pl.ds(0, 4), pl.ds(0, MAX_ROW)], sem.at[0])
        wait_bytes(sums.at[pl.ds(0, 3)], sem.at[1])

    def final_place(origin, k, core):
        tile, row, rows, _ = UNITS[k]
        at = (origin * 2 + core) * ROWS + row
        if tile < TILES:
            return out_q.at[pl.ds(pl.multiple_of(at, STEP), rows), pl.ds(tile * LANES, LANES)]
        return out_kv.at[:, pl.ds(pl.multiple_of(at, HALF), rows)]

    def kv_part(origin, k, last):
        first, columns = (LANES, HALF - LANES) if last else (0, LANES)
        at = origin * 2 * ROWS + UNITS[k][1] + first
        return out_kv.at[:, pl.ds(pl.multiple_of(at, LANES), columns)]

    def place(origin, k):
        tile, row, rows, _ = UNITS[k]
        return coded.at[origin, tile, pl.ds(row, rows)] if k < len(CODED) else final_place(origin, k, c)

    def unit_copy(ref, recv_sem, device, sem=send_sem):
        return pltpu.make_async_remote_copy(
            src_ref=ref, dst_ref=ref, send_sem=sem, recv_sem=recv_sem, device_id=device, device_id_type=MESH
        )

    def wait_units(units, sem):
        rows = sum(64 * HALF // LANES if k >= KV_UNITS[0] else UNITS[k][2] for k in units)
        wait_bytes(out_q.at[pl.ds(0, rows), pl.ds(0, LANES)], sem)

    to_right, to_left = {"zero_0": right}, {"zero_0": left}

    def send_right(k):
        unit_copy(place(x, k), side_recv.at[0, SIDE_OF[k]], to_right).start()

    def send_left(k):
        unit_copy(place(x, k), side_recv.at[1, SIDE_OF[k]], to_left).start()

    def relay(origin, k):
        unit_copy(final_place(origin, k, c), rel_recv, partner).start()

    def encode_rows(k, scale):
        tile, row, rows, _ = UNITS[k]
        cols = pl.ds(tile * LANES, LANES)

        def body(i, carry):
            at = pl.ds(pl.multiple_of(row + i * STEP, STEP), STEP)
            coded[x, tile, at, :] = encode(res_q[at, cols], scale)
            return carry

        lax.fori_loop(0, rows // STEP, body, 0)

    def decode_rows(origin, k, scales):
        tile, row, rows, _ = UNITS[k]
        cols = pl.ds(tile * LANES, LANES)
        own = sums[origin * 2 + c, MAX_ROW + (2 if tile else int(rows != FIRST))] * scales[tile]

        def body(i, carry):
            at = pl.multiple_of(row + i * STEP, STEP)
            there = pl.ds(pl.multiple_of((origin * 2 + c) * ROWS + at, STEP), STEP)
            out_q[there, cols] = (decode(coded[origin, tile, pl.ds(at, STEP), :]) * own).astype(jnp.bfloat16)
            return carry

        lax.fori_loop(0, rows // STEP, body, 0)

    lane_of = lax.broadcasted_iota(jnp.int32, (KV, LANES), 1)
    diagonal = lane_of == lax.broadcasted_iota(jnp.int32, (KV, LANES), 0)

    acc, scale = sum_first(0, nothing)
    encode_rows(0, scale)
    encode_rows(2, scale)
    wait_for_neighbours()
    send_right(0)
    send_left(2)
    acc, scale = sum_first(1, acc)
    encode_rows(1, scale)
    send_right(1)
    encode_rows(3, scale)
    for k in (3, 0, 1):
        send_left(k)
    for k in (2, 3):
        send_right(k)
    sums[me, 0] = jnp.sum(acc, axis=0, keepdims=True)
    scale = sum_tile(1)
    wait_bytes(wq_v.at[pl.ds(0, 4 * 32 * ROWS // COLS), :], in_sem.at[KV_ROW + 1])
    acc = jnp.zeros((KV, LANES), jnp.float32)
    for j in range(ROWS // LANES):
        cols = pl.ds(j * LANES, LANES)
        r = mix(skv_v[:, cols], wkv_v[:, cols])
        res_kv[:, cols] = r
        acc = acc + jnp.abs(r)
    row_sums = jnp.sum(acc, axis=1, keepdims=True)
    sums[me, KV_ROW] = jnp.sum(jnp.where(diagonal, row_sums, 0.0), axis=0, keepdims=True)
    wait_bytes(norm_v, in_sem.at[NORM_ROW + 1])
    own_norm = norm_v[0] + norm_v[1]
    sums[me, NORM_ROW] = jnp.concatenate([own_norm, own_norm], axis=1)
    for t in range(2, TILES):
        sum_tile(t)
    wait_for_far()
    send_sums()
    encode_rows(4, scale)
    encode_rows(5, scale)
    for k in (4, 5):
        send_right(k)
    for k in (5, 4):
        send_left(k)

    def factor_of(t):
        total = sums[0, t]
        for other in range(1, 8):
            total = total + sums[other, t]
        return total * (1.0 / D_MODEL)

    def narrow_tile(t):
        factor = factor_of(t)
        if t < TILES:
            fac_q[:, pl.ds(t * LANES, LANES)] = factor
            scale = 1.0 / factor
        else:
            fac_k[...] = factor[:, 0:32]
            fac_v[...] = pltpu.roll(factor, LANES - 32, 1)[:, 0:32]
            spread = jnp.sum(jnp.where(diagonal, jnp.broadcast_to(factor, (KV, LANES)), 0.0), axis=1, keepdims=True)
            scale = 1.0 / jnp.broadcast_to(spread, (KV, LANES))
        for half in range(2):
            if t < TILES:
                cols = pl.ds(t * LANES, LANES)

                def body(i, carry):
                    at = half * HALF + i * STEP
                    rows = pl.ds(pl.multiple_of(at, STEP), STEP)
                    there = pl.ds(pl.multiple_of(me * ROWS + at, STEP), STEP)
                    out_q[there, cols] = (res_q[rows, cols] * scale).astype(jnp.bfloat16)
                    return carry

                lax.fori_loop(0, HALF // STEP, body, 0)
            else:
                for j in range(HALF // LANES):
                    at = half * HALF + j * LANES
                    there = pl.ds(pl.multiple_of(me * ROWS + at, LANES), LANES)
                    out_kv[:, there] = (res_kv[:, pl.ds(at, LANES)] * scale).astype(jnp.bfloat16)
            for k in range(FIRST_OF[t], len(UNITS)):
                if UNITS[k][0] == t and UNITS[k][3] == half:
                    for go_there in (send_right, send_left) if half == 0 else (send_left, send_right):
                        go_there(k)
                    relay(x, k)

    wait_sums(sum_recv)
    for t in range(CODED_TILES, TILES + 1):
        narrow_tile(t)
    scales = []
    for t in range(CODED_TILES):
        factor = factor_of(t)
        fac_q[:, pl.ds(t * LANES, LANES)] = factor
        scales.append(1.0 / (CODE * factor))
    for k in range(len(CODED)):
        decode_rows(x, k, scales)
        relay(x, k)

    def norm_copy(buf, at, stage, device):
        return pltpu.make_async_remote_copy(
            src_ref=buf.at[at],
            dst_ref=buf.at[at],
            send_sem=norm_send,
            recv_sem=norm_recv.at[stage],
            device_id=device,
            device_id_type=MESH,
        )

    def norm_along_y():
        pl.semaphore_wait(barrier, 6)
        for other in range(8):
            norm_y[y, pl.ds(other, 1), :] = sums[other, NORM_ROW]
        for d in (2, 1, 3):
            norm_copy(norm_y, y, 0, {"width_1": lax.rem(y + d, 4)}).start()

    def norm_along_z():
        wait_bytes(norm_y.at[pl.ds(0, 3)], norm_recv.at[0])
        low = lax.broadcasted_iota(jnp.int32, (8, LANES), 1) < 64
        norm_z[z, 0] = jnp.where(low, norm_y[0], norm_y[1])
        norm_z[z, 1] = jnp.where(low, norm_y[2], norm_y[3])
        for d in (2, 1, 3):
            norm_copy(norm_z, z, 1, {"width_0": lax.rem(z + d, 4)}).start()

    def norm_end():
        wait_bytes(norm_z.at[pl.ds(0, 3)], norm_recv.at[1])
        for zz in range(4):
            for pair in range(2):
                for other in range(8):
                    norm_all[pl.ds(other * 8 + zz * 2 + pair, 1), :] = norm_z[zz, pair, pl.ds(other, 1), :]
        norm_out[...] = norm_all[...].astype(jnp.bfloat16)

    def norm_give():
        norm_to_partner().start()

    def norm_to_partner():
        return norm_copy(norm_out, pl.ds(0, 64), 2, partner)

    far = lax.rem(x + 2, 4)
    norm_steps = {1: norm_along_y, 2: norm_along_z, 3: norm_end}

    def hand_on(origin, k):
        if k < len(CODED):
            decode_rows(origin, k, scales)
        relay(origin, k)

    def forward(origin, k):
        unit_copy(place(origin, k), far_recv.at[FAR_OF[k]], to_left if UNITS[k][3] else to_right).start()

    for i in range(len(SIDE_GROUPS)):
        for side in range(2):
            group = i if i > 1 or side == 0 else 1 - i
            units, origin = SIDE_GROUPS[group], left if side == 0 else right
            wait_units(units, side_recv.at[side, group])
            for k in units:
                if UNITS[k][3] == side and k in KV_UNITS:

                    @pl.when(c == 1)
                    def _():
                        forward(origin, k)
                        relay(origin, k)

                    @pl.when(c == 0)
                    def _():
                        unit_copy(final_place(origin, k, 0), kv_recv, partner).start()
                    continue
                if UNITS[k][3] == side:
                    forward(origin, k)
                hand_on(origin, k)
        if i in norm_steps:
            pl.when(c == 0)(norm_steps[i])

    @pl.when(c == 1)
    def _():
        wait_units(KV_UNITS, kv_recv)
        for side, origin, device in ((0, left, to_right), (1, right, to_left)):
            k = KV_UNITS[side]
            unit_copy(kv_part(origin, k, False), far_kv_recv.at[0], device, extra_send).start()
            for core in range(2):
                to = {**device, "zero_1": core}
                unit_copy(kv_part(origin, k, True), far_kv_recv.at[1], to, extra_send).start()

    pl.when(c == 0)(norm_give)
    pl.when(c == 0)(lambda: wait_bytes(out_q.at[pl.ds(0, 9 * 16 + 64), pl.ds(0, LANES)], norm_send))
    pl.when(c == 1)(lambda: norm_to_partner().wait_recv())
    for group, units in enumerate(FAR_GROUPS):
        if units[0] in KV_UNITS:
            continue
        wait_units(units, far_recv.at[group])
        for k in units:
            hand_on(far, k)

    @pl.when(c == 1)
    def _():
        for k in KV_UNITS:
            wait_units((k,), far_recv.at[FAR_OF[k]])
            relay(far, k)
        wait_bytes(out_kv.at[:, pl.ds(0, 2 * LANES)], far_kv_recv.at[0])
        for k in KV_UNITS:
            unit_copy(kv_part(far, k, False), rel_recv, partner, extra_send).start()

    wait_bytes(out_kv.at[:, pl.ds(0, 2 * (HALF - LANES))], far_kv_recv.at[1])

    share = ROWS + KV * ROWS // COLS
    kv_rows = KV * ROWS // COLS

    wait_sums(sum_send)

    @pl.when(c == 1)
    def _():
        wait_bytes(out_q.at[pl.ds(0, 7 * share), :], send_sem)
        wait_bytes(out_q.at[pl.ds(0, 2 * kv_rows), :], extra_send)
        wait_bytes(out_q.at[pl.ds(0, 4 * share - 2 * kv_rows), :], rel_recv)

    @pl.when(c == 0)
    def _():
        wait_bytes(out_q.at[pl.ds(0, 7 * share - 2 * kv_rows), :], send_sem)
        wait_bytes(out_q.at[pl.ds(0, 4 * share + kv_rows // 4), :], rel_recv)


def write_kernel(
    out_q, out_kv, res_q, res_kv, fac_q, fac_k, fac_v, norm,
    final_q, final_k, final_v, factor_q, factor_k, factor_v, serve_norm, result_q, result_k, result_v, sem,
):
    def write(src, dst, which):
        pltpu.make_async_copy(src, dst, sem.at[which]).start()

    small = ((fac_q, factor_q), (fac_k, factor_k), (fac_v, factor_v), (norm, serve_norm))
    for i, (src, dst) in enumerate(small):
        write(src, dst, i)
    for part in range(8):
        rows = pl.ds(part * ROWS, ROWS)
        write(out_q.at[rows, :], final_q.at[rows, :], 4)
    write(res_q, result_q, 5)
    write(out_kv.at[pl.ds(0, 32), :], final_k, 6)
    write(out_kv.at[pl.ds(32, 32), :], final_v, 6)
    write(res_kv.at[pl.ds(0, 32), :], result_k, 7)
    write(res_kv.at[pl.ds(32, 32), :], result_v, 7)
    for i, ref in enumerate((fac_q, fac_k, fac_v, norm, out_q, res_q, out_kv, res_kv)):
        pltpu.make_async_copy(ref, ref, sem.at[i]).wait()


def on_device(weight_query, smooth_query, weight_key, smooth_key, weight_value, smooth_value, norm_train, norm_step):
    f32, bf16 = jnp.float32, jnp.bfloat16
    any_spec, vmem_spec = pl.BlockSpec(memory_space=pl.ANY), pl.BlockSpec(memory_space=pltpu.VMEM)
    held = (
        ((D_MODEL, COLS), bf16),
        ((KV, D_MODEL), bf16),
        ((ROWS, COLS), f32),
        ((KV, ROWS), f32),
        ((1, COLS), f32),
        ((1, 32), f32),
        ((1, 32), f32),
        ((64, LANES), bf16),
    )
    dma = pltpu.SemaphoreType.DMA
    gathered = pl.pallas_call(
        gather_kernel,
        out_shape=tuple(pltpu.VMEM(shape, dtype) for shape, dtype in held),
        in_specs=[any_spec] * 8,
        out_specs=tuple(vmem_spec for _ in held),
        scratch_shapes=[
            pltpu.VMEM((ROWS, COLS), f32),
            pltpu.VMEM((ROWS, COLS), f32),
            pltpu.VMEM((KV, ROWS), f32),
            pltpu.VMEM((KV, ROWS), f32),
            pltpu.VMEM((2, 1, 64), f32),
            pltpu.VMEM((4, CODED_TILES, ROWS, LANES), bf16),
            pltpu.VMEM((8, SUM_ROWS, 1, LANES), f32),
            pltpu.VMEM((4, 8, LANES), f32),
            pltpu.VMEM((4, 2, 8, LANES), f32),
            pltpu.VMEM((64, LANES), f32),
            dma((NORM_ROW + 2,)),
            dma,
            dma,
            dma((2,)),
            dma((2,)),
            dma((2, len(SIDE_GROUPS))),
            dma((len(FAR_GROUPS),)),
            dma,
            dma,
            dma((2,)),
            dma,
            dma((3,)),
            pltpu.SemaphoreType.REGULAR((2,)),
            pltpu.SemaphoreType.REGULAR,
        ],
        compiler_params=pltpu.CompilerParams(
            collective_id=0, has_side_effects=True, vmem_limit_bytes=16 * 1024 * 1024
        ),
        name="gather",
    )(
        *(
            pltpu.with_memory_space_constraint(a, pltpu.HBM)
            for a in (
                weight_query, smooth_query, weight_key.T, smooth_key.T, weight_value.T, smooth_value.T,
                norm_train.reshape(1, 64), norm_step.reshape(1, 64),
            )
        )
    )
    outs = (
        ((D_MODEL, COLS), bf16),
        ((32, D_MODEL), bf16),
        ((32, D_MODEL), bf16),
        ((1, COLS), f32),
        ((1, 32), f32),
        ((1, 32), f32),
        ((64, LANES), bf16),
        ((ROWS, COLS), f32),
        ((32, ROWS), f32),
        ((32, ROWS), f32),
    )
    fq, fk, fv, cq, ck, cv, norm, rq, rk, rv = pl.pallas_call(
        write_kernel,
        out_shape=tuple(jax.ShapeDtypeStruct(shape, dtype) for shape, dtype in outs),
        in_specs=[vmem_spec] * len(held),
        out_specs=tuple(any_spec for _ in outs),
        scratch_shapes=[dma((8,))],
        compiler_params=pltpu.CompilerParams(vmem_limit_bytes=4 * 1024 * 1024),
        name="write",
    )(*gathered)
    return (
        fq, fk.T, fv.T, cq.reshape(COLS), ck.reshape(32), cv.reshape(32), norm.reshape(D_MODEL), rq, rk.T, rv.T
    )


def solution(mesh):
    split = Mesh(mesh.devices.reshape(4, 2, 4, 4), ("zero_0", "zero_1", "width_0", "width_1"))
    in_specs = (
        P(ZERO, WIDTH),
        P(ZERO, WIDTH),
        P(ZERO, WIDTH),
        P(ZERO, WIDTH),
        P(ZERO, WIDTH),
        P(ZERO, WIDTH),
        P(ZERO_WIDTH),
        P(ZERO_WIDTH),
    )
    out_specs = (
        P(None, WIDTH),
        P(None, WIDTH),
        P(None, WIDTH),
        P(WIDTH),
        P(WIDTH),
        P(WIDTH),
        P(),
        P(ZERO, WIDTH),
        P(ZERO, WIDTH),
        P(ZERO, WIDTH),
    )
    return jax.shard_map(
        on_device, mesh=split, in_specs=in_specs, out_specs=out_specs, check_vma=False
    )
```
